32 devices in a mesh: seq: 8 (over y, x, core), fsdp: 4 (over z).
Axes of the slice: x: 2, y: 2, z: 4, core: 2. Of those that a mesh axis runs over, the one named last changes fastest.
Arguments:
- stream: float32 [4, 1024, 2048], P('fsdp', 'seq'), may hold values from -6 to 6
- segments: int32 [4, 1024], P('fsdp'), may hold values from 0 to 3, never falling along the last dimension, each value on 1 to 512 neighbouring positions
- attention_weights: float32 [2048, 8192], P(('seq', 'fsdp')), may hold values from -4 to 4
- feedforward_weights: float32 [2048, 16896], P(('seq', 'fsdp')), may hold values from -4 to 4
- norm_vectors: float32 [7, 2048], P(None, ('seq', 'fsdp')), may hold values from -2 to 2
- attention_moments: float32 [2, 2048, 8192], P(None, ('seq', 'fsdp')), may hold values from -1 to 1, as said below
- feedforward_moments: float32 [2, 2048, 16896], P(None, ('seq', 'fsdp')), may hold values from -1 to 1, as said below
- vector_moments: float32 [2, 7, 2048], P(None, None, ('seq', 'fsdp')), may hold values from -1 to 1, as said below
- cotangent: float32 [4, 1024, 2048], P('fsdp', 'seq'), may hold values from -1 to 1
Outputs:
- output_stream: float32 [4, 1024, 2048], P('fsdp', 'seq')
- stream_grad: float32 [4, 1024, 2048], P('fsdp', 'seq')
- attention_grad: float32 [2048, 8192], P(('seq', 'fsdp'))
- feedforward_grad: float32 [2048, 16896], P(('seq', 'fsdp'))
- vector_grad: float32 [7, 2048], P(None, ('seq', 'fsdp'))
- attention_new: float32 [2048, 8192], P(('seq', 'fsdp'))
- feedforward_new: float32 [2048, 16896], P(('seq', 'fsdp'))
- vector_new: float32 [7, 2048], P(None, ('seq', 'fsdp'))
- attention_state: float32 [2, 2048, 8192], P(None, ('seq', 'fsdp'))
- feedforward_state: float32 [2, 2048, 16896], P(None, ('seq', 'fsdp'))
- vector_state: float32 [2, 7, 2048], P(None, None, ('seq', 'fsdp'))
The draws below stay inside these ranges and needn't reach their ends.
Inputs may be any that keep to these rules, and one draw needn't show every extreme that they name: `segments`: segment numbers never fall along a sequence; every one of the 4 documents is present. `attention_moments`: the second moments (index 1 of the first dimension) lie within 0.01 to 0.1. `feedforward_moments`: the second moments (index 1 of the first dimension) lie within 0.01 to 0.1. `vector_moments`: the second moments (index 1 of the first dimension) lie within 0.01 to 0.1.
All inputs are finite; a program needn't handle non-finite values.
Results may differ from the reference program's by a relative error of at most 0.025.
The reference program's roundings to bfloat16 on the way count: a program that leaves them out, or rounds other values in their place, can miss the bound.
Values may be sent and summed in bfloat16 or wider, within the bound.
A program may use at most 384 MiB of HBM per device.

```python
import math
import jax
import jax.numpy as jnp
import numpy as np
from jax import lax

D = 2048
H = 32
HD = 64
ROT = 16
FF = 5632
DOCS = 4
SEQ_LEN = 1024
SEQS = 4


def draw_attention_weights(key, part):
    normal_vals = jax.random.truncated_normal(key, -4.0, 4.0, (D, 4 * D), jnp.float32)
    columns = jnp.arange(4 * D, dtype=jnp.int32)[None, :]
    query_factor = 1.0
    factor = jnp.where(columns < 2 * D, query_factor, jnp.where(columns >= 3 * D, 4.0, 1.0))
    return normal_vals * factor * float(D) ** (-0.5)


def draw_feedforward_weights(key, part):
    normal_vals = jax.random.truncated_normal(key, -4.0, 4.0, (D, 3 * FF), jnp.float32)
    columns = jnp.arange(3 * FF, dtype=jnp.int32)[None, :]
    return normal_vals * jnp.where(columns < 2 * FF, float(D) ** (-0.5), float(FF) ** (-0.5))


def draw_norm_vectors(key, part):
    row_ids = jnp.arange(7, dtype=jnp.int32)[:, None]
    gains = 1.0 + 0.12 * jax.random.truncated_normal(jax.random.fold_in(key, 1), -2.5, 2.5, (7, D), jnp.float32)
    shifts = 0.5 * jax.random.truncated_normal(jax.random.fold_in(key, 2), -4.0, 4.0, (7, D), jnp.float32)
    is_gain = (row_ids == 0) | (row_ids == 5)
    return jnp.where(is_gain, gains, shifts)


def moment_pair(key, shape):
    first = 0.25 * jax.random.truncated_normal(jax.random.fold_in(key, 11), -4.0, 4.0, shape, jnp.float32)
    second = jnp.exp(jax.random.uniform(jax.random.fold_in(key, 12), shape, jnp.float32, math.log(0.01), math.log(0.1)))
    return jnp.stack([first, second])


def draw_attention_moments(key, part):
    return moment_pair(key, (D, 4 * D))


def draw_feedforward_moments(key, part):
    return moment_pair(key, (D, 3 * FF))


def draw_vector_moments(key, part):
    return moment_pair(key, (7, D))


def draw_cotangent(key, part):
    factor = 0.6 / math.sqrt(float(SEQS * SEQ_LEN))
    values = jax.random.truncated_normal(key, -6.0, 6.0, (SEQS, SEQ_LEN, D), jnp.float32)
    return values * factor


def block_scale(key, extent, pieces, least, high):
    def one(axis_at, parts):
        steps = jax.random.uniform(jax.random.fold_in(jax.random.fold_in(key, 6), axis_at), (parts,), jnp.float32, least / len(pieces), high / len(pieces))
        return jnp.repeat(jnp.exp(steps), extent[axis_at] // parts).reshape((-1,) + (1,) * (len(extent) - axis_at - 1))

    loudness = one(*pieces[0])
    for cut in pieces[1:]:
        loudness = loudness * one(*cut)
    return loudness


def split_up(amount, total, reach, lean):
    loads = [(1 << 20) // math.isqrt(standing ** lean) + 1 for standing in range(2, amount + 1)]
    surplus, counts = total - reach - (amount - 1), [1] * (amount - 1)
    while surplus > 0:
        free = [i for i in range(amount - 1) if counts[i] < reach]
        pool, left = sum([loads[i] for i in free]), surplus
        for i in free:
            addition = min(reach - counts[i], max(1, left * loads[i] // pool), surplus)
            counts[i] = counts[i] + addition
            surplus = surplus - addition
    return np.array([reach] + counts)


def uneven_parts(rng, amount, total, limit, lean):
    if amount == 2:
        one = jax.random.randint(rng, (), max(1, total - limit), min(limit, total - 1) + 1)
        return jnp.stack([one, total - one])
    sizes = jnp.asarray(split_up(amount, total, limit, lean), jnp.int32)
    couples = (amount - 1) // 2
    source_of, sink = sizes[1:1 + 2 * couples:2], sizes[2:2 + 2 * couples:2]
    slack = jnp.minimum(source_of - 1, limit - sink)
    shifted = jax.random.randint(jax.random.fold_in(rng, 1), (couples,), 0, 1 << 20) % (slack + 1)
    sizes = sizes.at[1:1 + 2 * couples:2].set(source_of - shifted).at[2:2 + 2 * couples:2].set(sink + shifted)
    return sizes[jax.random.permutation(jax.random.fold_in(rng, 2), amount)]


def normal_values(key, shape, deviation, bound, pieces=(), held_as=jnp.bfloat16):
    entries = deviation * jax.random.normal(key, shape, jnp.float32)
    if pieces:
        entries = entries * block_scale(key, shape, pieces, -0.22, 0.18)
    return jnp.clip(entries, -bound, bound).astype(held_as)


def setup_inputs(seed: int = 0) -> dict:
    arg_keys = jax.random.split(jax.random.key(seed), 10)
    stream = normal_values(arg_keys[0], (SEQS, SEQ_LEN, D), 1.0, 6.0, ((0, 4), (1, 8)), jnp.float32)
    segments = jax.vmap(lambda own: jnp.searchsorted(jnp.cumsum(uneven_parts(own, DOCS, SEQ_LEN, SEQ_LEN // 2, 0)), jnp.arange(SEQ_LEN), side="right"))(jax.random.split(arg_keys[1], SEQS)).reshape((SEQS, SEQ_LEN)).astype(jnp.int32)
    attention_weights = draw_attention_weights(jax.random.fold_in(arg_keys[9], 71), 0)
    feedforward_weights = draw_feedforward_weights(jax.random.fold_in(arg_keys[9], 71), 0)
    norm_vectors = draw_norm_vectors(jax.random.fold_in(arg_keys[9], 71), 0)
    attention_moments = draw_attention_moments(jax.random.fold_in(arg_keys[9], 71), 0)
    feedforward_moments = draw_feedforward_moments(jax.random.fold_in(arg_keys[9], 71), 0)
    vector_moments = draw_vector_moments(jax.random.fold_in(arg_keys[9], 71), 0)
    cotangent = draw_cotangent(jax.random.fold_in(arg_keys[9], 71), 0)
    return {"stream": stream, "segments": segments, "attention_weights": attention_weights, "feedforward_weights": feedforward_weights, "norm_vectors": norm_vectors, "attention_moments": attention_moments, "feedforward_moments": feedforward_moments, "vector_moments": vector_moments, "cotangent": cotangent}


norm_epsilon = 1e-05
rope_base = 10000.0
neg_fill = -1e+30
learn_rate = 0.01
beta_first = 0.9
beta_second = 0.95
adam_epsilon = 1e-08
decay_rate = 0.1
adam_step = 2.0

def document_positions(segment_ids):
    length = segment_ids.shape[0]
    indices = jnp.arange(length, dtype=jnp.int32)
    changes = jnp.concatenate([jnp.ones((1,), dtype=jnp.bool_), segment_ids[1:] != segment_ids[:-1]])
    starts = lax.cummax(jnp.where(changes, indices, jnp.zeros_like(indices)), axis=0)
    return indices - starts

def rotary_tables(positions, half_rot):
    powers = jnp.arange(half_rot, dtype=jnp.float32) / float(half_rot)
    inverse = rope_base ** (-powers)
    angles = positions.astype(jnp.float32)[:, None] * inverse[None, :]
    return (jnp.cos(angles), jnp.sin(angles))

def rotate(values, cosine, sine, half_rot, direction):
    first = values[..., :half_rot]
    second = values[..., half_rot:2 * half_rot]
    cosine_wide = cosine[:, None, :]
    sine_wide = sine[:, None, :] * direction
    return jnp.concatenate([first * cosine_wide - second * sine_wide, second * cosine_wide + first * sine_wide, values[..., 2 * half_rot:]], axis=-1)

def norm_forward(values, gain, shift):
    centred = values - lax.optimization_barrier(jnp.mean(values, axis=-1, keepdims=True))
    inverse = lax.rsqrt(lax.optimization_barrier(jnp.mean(centred * centred, axis=-1, keepdims=True)) + norm_epsilon)
    normal_part = centred * inverse
    return (normal_part * gain + shift, normal_part, inverse)

def norm_backward(upstream, normal_part, inverse, gain):
    scaled = upstream * gain
    return inverse * (scaled - lax.optimization_barrier(jnp.mean(scaled, axis=-1, keepdims=True)) - normal_part * lax.optimization_barrier(jnp.mean(scaled * normal_part, axis=-1, keepdims=True)))

def head_scores(query_head, key_head, segment_ids):
    length = query_head.shape[0]
    scores = jnp.dot(query_head, key_head.T, preferred_element_type=jnp.float32) * float(HD) ** (-0.5)
    indices = jnp.arange(length, dtype=jnp.int32)
    allowed = (indices[None, :] <= indices[:, None]) & (segment_ids[None, :] == segment_ids[:, None])
    return jnp.where(allowed, scores, neg_fill)

def head_forward(query_head, key_head, value_head, segment_ids):
    scores = head_scores(query_head, key_head, segment_ids)
    row_max = lax.optimization_barrier(jnp.max(scores, axis=-1, keepdims=True))
    weights_raw = jnp.exp(scores - row_max)
    row_sum = lax.optimization_barrier(jnp.sum(weights_raw, axis=-1, keepdims=True))
    probability = (weights_raw / row_sum).astype(jnp.bfloat16)
    output_head = jnp.dot(probability, value_head, preferred_element_type=jnp.float32).astype(jnp.bfloat16)
    return (output_head, (row_max + jnp.log(row_sum))[:, 0])

def head_backward(query_head, key_head, value_head, output_head, grad_head, logsum, segment_ids):
    scores = head_scores(query_head, key_head, segment_ids)
    probability = jnp.exp(scores - logsum[:, None])
    prob_low = probability.astype(jnp.bfloat16)
    grad_value = jnp.dot(prob_low.T, grad_head, preferred_element_type=jnp.float32).astype(jnp.bfloat16)
    grad_prob = jnp.dot(grad_head, value_head.T, preferred_element_type=jnp.float32)
    row_delta = lax.optimization_barrier(jnp.sum(grad_head.astype(jnp.float32) * output_head.astype(jnp.float32), axis=-1, keepdims=True))
    grad_scores = (probability * (grad_prob - row_delta) * float(HD) ** (-0.5)).astype(jnp.bfloat16)
    grad_query = jnp.dot(grad_scores, key_head, preferred_element_type=jnp.float32).astype(jnp.bfloat16)
    grad_key = jnp.dot(grad_scores.T, query_head, preferred_element_type=jnp.float32).astype(jnp.bfloat16)
    return (grad_query, grad_key, grad_value)

def heads_first(values):
    return jnp.transpose(values, (1, 0, 2))

def sequence_pass(inputs, segment_ids, upstream, attention_low, feedforward_low, vector_full):
    length = inputs.shape[0]
    half_rot = ROT // 2
    gain_one, shift_one, bias_query, bias_key, bias_value, gain_two, shift_two = [vector_full[row_index] for row_index in range(7)]
    cosine, sine = rotary_tables(document_positions(segment_ids), half_rot)
    normed_one, normal_one, inverse_one = norm_forward(inputs, gain_one, shift_one)
    normed_low = normed_one.astype(jnp.bfloat16)
    projected = jnp.dot(normed_low, attention_low[:, :3 * D], preferred_element_type=jnp.float32) + jnp.concatenate([bias_query, bias_key, bias_value])
    query_rot = rotate(projected[:, :D].reshape(length, H, HD), cosine, sine, half_rot, 1.0).astype(jnp.bfloat16)
    key_rot = rotate(projected[:, D:2 * D].reshape(length, H, HD), cosine, sine, half_rot, 1.0).astype(jnp.bfloat16)
    value_low = projected[:, 2 * D:].reshape(length, H, HD).astype(jnp.bfloat16)
    query_heads = heads_first(query_rot)
    key_heads = heads_first(key_rot)
    value_heads = heads_first(value_low)
    output_heads, logsum = lax.map(lambda items: head_forward(items[0], items[1], items[2], segment_ids), (query_heads, key_heads, value_heads))
    attended = heads_first(output_heads).reshape(length, D)
    hidden = inputs + jnp.dot(attended, attention_low[:, 3 * D:], preferred_element_type=jnp.float32)
    normed_two, normal_two, inverse_two = norm_forward(hidden, gain_two, shift_two)
    normed_low_two = normed_two.astype(jnp.bfloat16)
    gate_up = jnp.dot(normed_low_two, feedforward_low[:, :2 * FF], preferred_element_type=jnp.float32)
    gate_part = gate_up[:, :FF]
    up_part = gate_up[:, FF:]
    sigmoid_gate = jax.nn.sigmoid(gate_part)
    activated = (gate_part * sigmoid_gate * up_part).astype(jnp.bfloat16)
    down_low = feedforward_low[:, 2 * FF:]
    result = hidden + jnp.dot(activated, down_low.T, preferred_element_type=jnp.float32)
    cotangent_low = upstream.astype(jnp.bfloat16)
    grad_down = jnp.dot(cotangent_low.T, activated, preferred_element_type=jnp.float32)
    grad_act = jnp.dot(cotangent_low, down_low, preferred_element_type=jnp.float32)
    grad_gate = grad_act * up_part * sigmoid_gate * (1.0 + gate_part * (1.0 - sigmoid_gate))
    grad_up = grad_act * gate_part * sigmoid_gate
    grad_gate_up = jnp.concatenate([grad_gate, grad_up], axis=1).astype(jnp.bfloat16)
    grad_in_proj = jnp.dot(normed_low_two.T, grad_gate_up, preferred_element_type=jnp.float32)
    grad_normed_two = jnp.dot(grad_gate_up, feedforward_low[:, :2 * FF].T, preferred_element_type=jnp.float32)
    grad_hidden = upstream + norm_backward(grad_normed_two, normal_two, inverse_two, gain_two)
    grad_gain_two = lax.optimization_barrier(jnp.sum(grad_normed_two * normal_two, axis=0))
    grad_shift_two = lax.optimization_barrier(jnp.sum(grad_normed_two, axis=0))
    grad_hidden_low = grad_hidden.astype(jnp.bfloat16)
    grad_out_proj = jnp.dot(attended.T, grad_hidden_low, preferred_element_type=jnp.float32)
    grad_attended = jnp.dot(grad_hidden_low, attention_low[:, 3 * D:].T, preferred_element_type=jnp.float32).astype(jnp.bfloat16)
    grad_heads = heads_first(grad_attended.reshape(length, H, HD))
    grad_query, grad_key, grad_value = lax.map(lambda items: head_backward(items[0], items[1], items[2], items[3], items[4], items[5], segment_ids), (query_heads, key_heads, value_heads, output_heads, grad_heads, logsum))
    grad_query_tok = rotate(heads_first(grad_query).astype(jnp.float32), cosine, sine, half_rot, -1.0).reshape(length, D)
    grad_key_tok = rotate(heads_first(grad_key).astype(jnp.float32), cosine, sine, half_rot, -1.0).reshape(length, D)
    grad_value_tok = heads_first(grad_value).astype(jnp.float32).reshape(length, D)
    grad_projected = jnp.concatenate([grad_query_tok, grad_key_tok, grad_value_tok], axis=1)
    grad_bias = lax.optimization_barrier(jnp.sum(grad_projected, axis=0))
    grad_projected_low = grad_projected.astype(jnp.bfloat16)
    grad_qkv_proj = jnp.dot(normed_low.T, grad_projected_low, preferred_element_type=jnp.float32)
    grad_normed_one = jnp.dot(grad_projected_low, attention_low[:, :3 * D].T, preferred_element_type=jnp.float32)
    grad_stream = grad_hidden + norm_backward(grad_normed_one, normal_one, inverse_one, gain_one)
    grad_gain_one = lax.optimization_barrier(jnp.sum(grad_normed_one * normal_one, axis=0))
    grad_shift_one = lax.optimization_barrier(jnp.sum(grad_normed_one, axis=0))
    attention_part = jnp.concatenate([grad_qkv_proj, grad_out_proj], axis=1)
    feedforward_part = jnp.concatenate([grad_in_proj, grad_down], axis=1)
    vector_part = jnp.stack([grad_gain_one, grad_shift_one, grad_bias[:D], grad_bias[D:2 * D], grad_bias[2 * D:], grad_gain_two, grad_shift_two])
    return (result, grad_stream, attention_part, feedforward_part, vector_part)

def adamw_update(weight, grad, moments, decay):
    first = beta_first * moments[0] + (1.0 - beta_first) * grad
    second = beta_second * moments[1] + (1.0 - beta_second) * grad * grad
    correct_one = 1.0 - beta_first ** adam_step
    correct_two = 1.0 - beta_second ** adam_step
    update = first / correct_one / (jnp.sqrt(second / correct_two) + adam_epsilon)
    return (weight - learn_rate * (update + decay * weight), jnp.stack([first, second]))

def reference(stream, segments, attention_weights, feedforward_weights, norm_vectors, attention_moments, feedforward_moments, vector_moments, cotangent):
    attention_low = attention_weights.astype(jnp.bfloat16)
    feedforward_low = feedforward_weights.astype(jnp.bfloat16)
    vector_full = norm_vectors.astype(jnp.bfloat16).astype(jnp.float32)

    def one_sequence(carry, items):
        result, grad_stream, attention_part, feedforward_part, vector_part = sequence_pass(items[0], items[1], items[2], attention_low, feedforward_low, vector_full)
        return ((carry[0] + attention_part, carry[1] + feedforward_part, carry[2] + vector_part), (result, grad_stream))
    start_carry = (jnp.zeros((D, 4 * D), jnp.float32), jnp.zeros((D, 3 * FF), jnp.float32), jnp.zeros((7, D), jnp.float32))
    totals, outputs = lax.scan(one_sequence, start_carry, (stream, segments, cotangent))
    attention_grad, feedforward_grad, vector_grad = totals
    output_stream, stream_grad = outputs
    attention_new, attention_state = adamw_update(attention_weights, attention_grad, attention_moments, decay_rate)
    feedforward_new, feedforward_state = adamw_update(feedforward_weights, feedforward_grad, feedforward_moments, decay_rate)
    vector_new, vector_state = adamw_update(norm_vectors, vector_grad, vector_moments, 0.0)
    return (output_stream, stream_grad, attention_grad, feedforward_grad, vector_grad, attention_new, feedforward_new, vector_new, attention_state, feedforward_state, vector_state)
```

```python
import functools

import jax
import jax.numpy as jnp
from jax import lax
from jax.experimental import pallas as pl
from jax.experimental.pallas import tpu as pltpu
from jax.sharding import PartitionSpec as P

D = 2048
H = 32
HD = 64
ROT = 16
FF = 5632

norm_epsilon = 1e-05
rope_base = 10000.0
neg_fill = -1e30
learn_rate = 0.01
beta_first = 0.9
beta_second = 0.95
adam_epsilon = 1e-08
decay_rate = 0.1
adam_step = 2.0

MESH_IDS = pl.DeviceIdType.MESH
bf16 = jnp.bfloat16
f32 = jnp.float32


def document_positions(segment_ids):
    length = segment_ids.shape[0]
    indices = jnp.arange(length, dtype=jnp.int32)
    changes = jnp.concatenate(
        [jnp.ones((1,), dtype=jnp.bool_), segment_ids[1:] != segment_ids[:-1]]
    )
    starts = lax.cummax(jnp.where(changes, indices, jnp.zeros_like(indices)), axis=0)
    return indices - starts


def rotary_tables(positions, half_rot):
    powers = jnp.arange(half_rot, dtype=jnp.float32) / float(half_rot)
    inverse = rope_base ** (-powers)
    angles = positions.astype(jnp.float32)[:, None] * inverse[None, :]
    return (jnp.cos(angles), jnp.sin(angles))


def rotate(values, cosine, sine, half_rot, direction):
    first = values[..., :half_rot]
    second = values[..., half_rot : 2 * half_rot]
    cosine_wide = cosine[:, None, :]
    sine_wide = sine[:, None, :] * direction
    return jnp.concatenate(
        [
            first * cosine_wide - second * sine_wide,
            second * cosine_wide + first * sine_wide,
            values[..., 2 * half_rot :],
        ],
        axis=-1,
    )


def norm_forward(values, gain, shift):
    centred = values - jnp.mean(values, axis=-1, keepdims=True)
    inverse = lax.rsqrt(jnp.mean(centred * centred, axis=-1, keepdims=True) + norm_epsilon)
    normal_part = centred * inverse
    return (normal_part * gain + shift, normal_part, inverse)


def norm_backward(upstream, normal_part, inverse, gain):
    scaled = upstream * gain
    return inverse * (
        scaled
        - jnp.mean(scaled, axis=-1, keepdims=True)
        - normal_part * jnp.mean(scaled * normal_part, axis=-1, keepdims=True)
    )


def contract_rows(left, right, out=jnp.float32):
    return lax.dot_general(left, right, (((0,), (0,)), ((), ())), preferred_element_type=out)


def contract_cols(left, right, out=jnp.float32):
    return lax.dot_general(left, right, (((1,), (1,)), ((), ())), preferred_element_type=out)


def block_mask(segment_ids, start_row, block_rows):
    total_keys = segment_ids.shape[0]
    row_ids = start_row + jnp.arange(block_rows, dtype=jnp.int32)
    col_ids = jnp.arange(total_keys, dtype=jnp.int32)
    row_segments = lax.dynamic_slice_in_dim(segment_ids, start_row, block_rows)
    return (col_ids[None, :] <= row_ids[:, None]) & (segment_ids[None, :] == row_segments[:, None])


def adamw_update(weight, grad, moments, decay):
    first = beta_first * moments[0] + (1.0 - beta_first) * grad
    second = beta_second * moments[1] + (1.0 - beta_second) * grad * grad
    correct_one = 1.0 - beta_first**adam_step
    correct_two = 1.0 - beta_second**adam_step
    update = first / correct_one / (jnp.sqrt(second / correct_two) + adam_epsilon)
    return (weight - learn_rate * (update + decay * weight), jnp.stack([first, second]))


def plane_places():
    me = lax.axis_index("seq")
    core = me % 2
    first = 2 + 2 * core
    second = 4 - 2 * core
    bit_first = (me // first) % 2
    bit_second = (me // second) % 2
    sibling = me + 1 - 2 * core
    near = me + first * (1 - 2 * bit_first)
    far = me + second * (1 - 2 * bit_second)
    corner = near + second * (1 - 2 * bit_second)
    return me, sibling, near, far, corner


def greet(others):
    barrier = pltpu.get_barrier_semaphore()
    for other in others:
        pl.semaphore_signal(barrier, inc=1, device_id={"seq": other}, device_id_type=MESH_IDS)
    pl.semaphore_wait(barrier, len(others))


def gather_kernel(x_ref, o_ref, local_sem, send_sem, recv_sem):
    me, sibling, near, far, corner = plane_places()

    def copy(source, slot, index, target):
        return pltpu.make_async_remote_copy(
            src_ref=source,
            dst_ref=o_ref.at[slot],
            send_sem=send_sem.at[index],
            recv_sem=recv_sem.at[index],
            device_id={"seq": target},
            device_id_type=MESH_IDS,
        )

    greet((sibling, near, far))
    own = pltpu.make_async_copy(x_ref, o_ref.at[me], local_sem)
    own.start()
    to_near = copy(x_ref, me, 0, near)
    to_far = copy(x_ref, me, 1, far)
    to_sibling = copy(x_ref, me, 2, sibling)
    to_near.start()
    to_far.start()
    to_sibling.start()
    to_near.wait_recv()
    near_far = copy(o_ref.at[near], near, 3, far)
    near_far.start()
    near_sibling = copy(o_ref.at[near], near, 4, sibling)
    near_sibling.start()
    to_far.wait_recv()
    far_sibling = copy(o_ref.at[far], far, 5, sibling)
    far_sibling.start()
    near_far.wait_recv()
    corner_sibling = copy(o_ref.at[corner], corner, 6, sibling)
    corner_sibling.start()
    for one in (to_sibling, near_sibling, far_sibling, corner_sibling):
        one.wait_recv()
    for one in (to_near, to_far, to_sibling, near_far, near_sibling, far_sibling, corner_sibling):
        one.wait_send()
    own.wait()


def plane_gather(values, collective_id):
    rows, cols = values.shape
    out = pl.pallas_call(
        gather_kernel,
        out_shape=jax.ShapeDtypeStruct((8, rows, cols), values.dtype),
        in_specs=[pl.BlockSpec(memory_space=pltpu.VMEM)],
        out_specs=pl.BlockSpec(memory_space=pl.ANY),
        scratch_shapes=[
            pltpu.SemaphoreType.DMA,
            pltpu.SemaphoreType.DMA((7,)),
            pltpu.SemaphoreType.DMA((7,)),
        ],
        compiler_params=pltpu.CompilerParams(collective_id=collective_id, has_side_effects=True),
        name="plane_gather",
    )(values)
    return out.reshape(8 * rows, cols)


def scatter_kernel(p_ref, o_ref, mine, pair, near_out, near_in, far_out, far_in, local_sem, send_sem, recv_sem):
    me, sibling, near, far, corner = plane_places()
    flip = sibling - me
    order = (corner, near, far, me)
    sibling_order = (corner, far, near, me)

    def copy(source, target_ref, index, target):
        return pltpu.make_async_remote_copy(
            src_ref=source,
            dst_ref=target_ref,
            send_sem=send_sem.at[index],
            recv_sem=recv_sem.at[index],
            device_id={"seq": target},
            device_id_type=MESH_IDS,
        )

    greet((sibling, near, far))
    pairs = []
    locals_ = []
    for index, block in enumerate(order):
        one = copy(p_ref.at[sibling_order[index] + flip], pair.at[index], index, sibling)
        one.start()
        pairs.append(one)
        own = pltpu.make_async_copy(p_ref.at[block], mine.at[index], local_sem.at[index])
        own.start()
        locals_.append(own)
    for index in range(2):
        pairs[index].wait_recv()
        locals_[index].wait()
        near_out[index] = (mine[index].astype(f32) + pair[index].astype(f32)).astype(near_out.dtype)
        step = copy(near_out.at[index], near_in.at[index], 4 + index, near)
        step.start()
        pairs.append(step)
    for index in range(2, 4):
        pairs[index].wait_recv()
        locals_[index].wait()
    pairs[4].wait_recv()
    far_out[...] = (
        mine[2].astype(f32) + pair[2].astype(f32) + near_in[0].astype(f32)
    ).astype(far_out.dtype)
    last = copy(far_out, far_in, 6, far)
    last.start()
    pairs[5].wait_recv()
    o_ref[...] = mine[3].astype(f32) + pair[3].astype(f32) + near_in[1].astype(f32)
    last.wait_recv()
    o_ref[...] += far_in[...].astype(f32)
    for one in pairs:
        one.wait_send()
    last.wait_send()


def plane_scatter(values, collective_id):
    rows, cols = values.shape
    rows = rows // 8
    return pl.pallas_call(
        scatter_kernel,
        out_shape=jax.ShapeDtypeStruct((rows, cols), f32),
        in_specs=[pl.BlockSpec(memory_space=pl.ANY)],
        out_specs=pl.BlockSpec(memory_space=pltpu.VMEM),
        scratch_shapes=[
            pltpu.VMEM((4, rows, cols), values.dtype),
            pltpu.VMEM((4, rows, cols), values.dtype),
            pltpu.VMEM((2, rows, cols), values.dtype),
            pltpu.VMEM((2, rows, cols), values.dtype),
            pltpu.VMEM((rows, cols), values.dtype),
            pltpu.VMEM((rows, cols), values.dtype),
            pltpu.SemaphoreType.DMA((4,)),
            pltpu.SemaphoreType.DMA((7,)),
            pltpu.SemaphoreType.DMA((7,)),
        ],
        compiler_params=pltpu.CompilerParams(
            collective_id=collective_id, has_side_effects=True, vmem_limit_bytes=32 << 20
        ),
        name="plane_scatter",
    )(values.reshape(8, rows, cols))


def gather_tokens(values, collective_id):
    if lax.axis_size("seq") == 8:
        return plane_gather(values, collective_id)
    return lax.all_gather(values, "seq", axis=0, tiled=True)


def scatter_tokens(values, collective_id):
    if lax.axis_size("seq") == 8:
        return plane_scatter(values.astype(bf16), collective_id)
    return lax.psum_scatter(values, "seq", scatter_dimension=0, tiled=True)


def body(
    stream,
    segments,
    attention_weights,
    feedforward_weights,
    norm_vectors,
    attention_moments,
    feedforward_moments,
    vector_moments,
    cotangent,
):
    groups = lax.axis_size("seq")
    shards = lax.axis_size("fsdp")
    my_rank = lax.axis_index("seq")
    tokens = stream.shape[1]
    length = tokens * groups
    local_heads = H // groups
    local_width = local_heads * HD
    unit_width = FF // groups
    owned_rows = D // (groups * shards)
    plane_rows = groups * owned_rows
    half_rot = ROT // 2
    score_scale = float(HD) ** (-0.5)
    block_rows = min(512, length)
    block_starts = jnp.arange(length // block_rows, dtype=jnp.int32) * block_rows

    def to_order(values):
        lead = values.shape[:-1]
        return values.reshape(*lead, groups, shards, owned_rows).swapaxes(-3, -2).reshape(*lead, D)

    def from_order(values):
        lead = values.shape[:-1]
        return values.reshape(*lead, shards, groups, owned_rows).swapaxes(-3, -2).reshape(*lead, D)

    def spread_columns(values, parts, width):
        blocks = values.reshape(owned_rows, parts, groups, width).transpose(2, 0, 1, 3)
        blocks = blocks.reshape(groups, owned_rows, parts * width)
        moved = lax.all_to_all(blocks, "seq", split_axis=0, concat_axis=0, tiled=True)
        return moved.reshape(plane_rows, parts * width)

    attention_low = attention_weights.astype(bf16)
    feedforward_low = feedforward_weights.astype(bf16)
    vector_low = lax.all_gather(norm_vectors.astype(bf16), ("seq", "fsdp"), axis=1, tiled=True)
    qkv_weights = lax.all_gather(
        spread_columns(attention_low[:, : 3 * D], 3, local_width), "fsdp", axis=0, tiled=True
    )
    out_weights = lax.all_gather(to_order(attention_low[:, 3 * D :]), "fsdp", axis=0, tiled=True)
    in_weights = lax.all_gather(
        spread_columns(feedforward_low[:, : 2 * FF], 2, unit_width), "fsdp", axis=0, tiled=True
    )
    down_weights = lax.all_gather(
        spread_columns(feedforward_low[:, 2 * FF :], 1, unit_width), "fsdp", axis=0, tiled=True
    )

    vector_full = vector_low.astype(f32)
    ordered = to_order(vector_full)
    gain_one, shift_one, gain_two, shift_two = [ordered[i] for i in (0, 1, 5, 6)]
    bias = lax.dynamic_slice_in_dim(
        vector_full[2:5], my_rank * local_width, local_width, axis=1
    ).reshape(3 * local_width)
    segment_ids = segments[0]
    cosine, sine = rotary_tables(document_positions(segment_ids), half_rot)

    inputs = to_order(stream[0])
    upstream = to_order(cotangent[0])
    normed_one, normal_one, inverse_one = norm_forward(inputs, gain_one, shift_one)
    normed_all = gather_tokens(normed_one.astype(bf16), 1)
    cotangent_all = gather_tokens(upstream.astype(bf16), 2)
    projected = (
        jnp.dot(normed_all, qkv_weights, preferred_element_type=f32) + bias
    ).reshape(length, 3, local_heads, HD)
    query_all = rotate(projected[:, 0], cosine, sine, half_rot, 1.0).astype(bf16)
    key_all = rotate(projected[:, 1], cosine, sine, half_rot, 1.0).astype(bf16)
    value_all = projected[:, 2].astype(bf16)

    def forward_block(start_row):
        query_block = lax.dynamic_slice_in_dim(query_all, start_row, block_rows)
        scores = (
            jnp.einsum("bhd,lhd->hbl", query_block, key_all, preferred_element_type=jnp.float32)
            * score_scale
        )
        scores = jnp.where(block_mask(segment_ids, start_row, block_rows)[None], scores, neg_fill)
        row_max = jnp.max(scores, axis=-1, keepdims=True)
        weights_raw = jnp.exp(scores - row_max)
        row_sum = jnp.sum(weights_raw, axis=-1, keepdims=True)
        probability = (weights_raw / row_sum).astype(jnp.bfloat16)
        output_block = jnp.einsum(
            "hbl,lhd->bhd", probability, value_all, preferred_element_type=jnp.float32
        ).astype(jnp.bfloat16)
        return (output_block, (row_max + jnp.log(row_sum))[..., 0])

    output_blocks, logsum_blocks = lax.map(forward_block, block_starts)
    output_heads = output_blocks.reshape(length, local_heads, HD)
    attended = output_heads.reshape(length, local_width)
    hidden = inputs + scatter_tokens(jnp.dot(attended, out_weights, preferred_element_type=f32), 3)
    normed_two, normal_two, inverse_two = norm_forward(hidden, gain_two, shift_two)
    normed_two_all = gather_tokens(normed_two.astype(bf16), 4)
    gate_up = jnp.dot(normed_two_all, in_weights, preferred_element_type=f32)
    gate_part = gate_up[:, :unit_width]
    up_part = gate_up[:, unit_width:]
    sigmoid_gate = jax.nn.sigmoid(gate_part)
    activated = (gate_part * sigmoid_gate * up_part).astype(bf16)
    grad_act = jnp.dot(cotangent_all, down_weights, preferred_element_type=f32)
    grad_gate = grad_act * up_part * sigmoid_gate * (1.0 + gate_part * (1.0 - sigmoid_gate))
    grad_up = grad_act * gate_part * sigmoid_gate
    grad_gate_up = jnp.concatenate([grad_gate, grad_up], axis=1).astype(bf16)
    grad_normed_two = scatter_tokens(contract_cols(grad_gate_up, in_weights), 5)

    def reduce_rows(term):
        return lax.psum_scatter(term.astype(bf16), "fsdp", scatter_dimension=0, tiled=True)

    def collect_rows(total, parts, width):
        moved = lax.all_to_all(
            total.reshape(groups, owned_rows, parts, width),
            "seq",
            split_axis=0,
            concat_axis=0,
            tiled=True,
        ).astype(f32)
        return moved.transpose(1, 2, 0, 3).reshape(owned_rows, parts * groups * width)

    down_sum = reduce_rows(contract_rows(cotangent_all, activated))
    in_sum = reduce_rows(contract_rows(normed_two_all, grad_gate_up))

    grad_hidden = upstream + norm_backward(grad_normed_two, normal_two, inverse_two, gain_two)
    grad_gain_two = jnp.sum(grad_normed_two * normal_two, axis=0)
    grad_shift_two = jnp.sum(grad_normed_two, axis=0)
    grad_hidden_all = gather_tokens(grad_hidden.astype(bf16), 6)
    grad_heads = (
        contract_cols(grad_hidden_all, out_weights).astype(bf16).reshape(length, local_heads, HD)
    )
    out_sum = reduce_rows(contract_rows(attended, grad_hidden_all))
    result = hidden + scatter_tokens(contract_cols(activated, down_weights), 7)

    def backward_block(carry, items):
        grad_key_sum, grad_value_sum = carry
        start_row, logsum_block = items
        query_block = lax.dynamic_slice_in_dim(query_all, start_row, block_rows)
        output_block = lax.dynamic_slice_in_dim(output_heads, start_row, block_rows)
        grad_block = lax.dynamic_slice_in_dim(grad_heads, start_row, block_rows)
        scores = (
            jnp.einsum("bhd,lhd->hbl", query_block, key_all, preferred_element_type=jnp.float32)
            * score_scale
        )
        scores = jnp.where(block_mask(segment_ids, start_row, block_rows)[None], scores, neg_fill)
        probability = jnp.exp(scores - logsum_block[..., None])
        prob_low = probability.astype(jnp.bfloat16)
        grad_value_sum = grad_value_sum + jnp.einsum(
            "hbl,bhd->lhd", prob_low, grad_block, preferred_element_type=jnp.float32
        )
        grad_prob = jnp.einsum(
            "bhd,lhd->hbl", grad_block, value_all, preferred_element_type=jnp.float32
        )
        row_delta = jnp.sum(
            grad_block.astype(jnp.float32) * output_block.astype(jnp.float32), axis=-1
        )
        row_delta = jnp.transpose(row_delta)[..., None]
        grad_scores = (probability * (grad_prob - row_delta) * score_scale).astype(jnp.bfloat16)
        grad_query = jnp.einsum(
            "hbl,lhd->bhd", grad_scores, key_all, preferred_element_type=jnp.float32
        ).astype(jnp.bfloat16)
        grad_key_sum = grad_key_sum + jnp.einsum(
            "hbl,bhd->lhd", grad_scores, query_block, preferred_element_type=jnp.float32
        )
        return ((grad_key_sum, grad_value_sum), grad_query)

    zero_heads = jnp.zeros((length, local_heads, HD), jnp.float32)
    sums, grad_query_blocks = lax.scan(
        backward_block, (zero_heads, zero_heads), (block_starts, logsum_blocks)
    )
    grad_key_sum, grad_value_sum = sums
    grad_query_low = grad_query_blocks.reshape(length, local_heads, HD)
    grad_projected = jnp.concatenate(
        [
            rotate(grad_query_low.astype(f32), cosine, sine, half_rot, -1.0).reshape(
                length, local_width
            ),
            rotate(
                lax.optimization_barrier(grad_key_sum.astype(bf16)).astype(f32),
                cosine,
                sine,
                half_rot,
                -1.0,
            ).reshape(length, local_width),
            lax.optimization_barrier(grad_value_sum.astype(bf16)).astype(f32).reshape(
                length, local_width
            ),
        ],
        axis=1,
    )
    grad_bias = jnp.sum(grad_projected, axis=0)
    grad_projected_low = grad_projected.astype(bf16)
    qkv_sum = reduce_rows(contract_rows(normed_all, grad_projected_low))
    grad_normed_one = scatter_tokens(contract_cols(grad_projected_low, qkv_weights), 8)
    grad_stream = grad_hidden + norm_backward(grad_normed_one, normal_one, inverse_one, gain_one)
    grad_gain_one = jnp.sum(grad_normed_one * normal_one, axis=0)
    grad_shift_one = jnp.sum(grad_normed_one, axis=0)

    feedforward_grad = jnp.concatenate(
        [collect_rows(in_sum, 2, unit_width), collect_rows(down_sum, 1, unit_width)], axis=1
    )
    attention_grad = jnp.concatenate(
        [collect_rows(qkv_sum, 3, local_width), from_order(out_sum.astype(f32))], axis=1
    )
    bias_rows = lax.dynamic_update_slice_in_dim(
        jnp.zeros((3, D), f32), grad_bias.reshape(3, local_width), my_rank * local_width, axis=1
    )
    vector_term = jnp.concatenate(
        [
            from_order(jnp.stack([grad_gain_one, grad_shift_one])),
            bias_rows,
            from_order(jnp.stack([grad_gain_two, grad_shift_two])),
        ]
    )
    vector_grad = lax.psum_scatter(vector_term, ("seq", "fsdp"), scatter_dimension=1, tiled=True)
    attention_new, attention_state = adamw_update(
        attention_weights, attention_grad, attention_moments, decay_rate
    )
    feedforward_new, feedforward_state = adamw_update(
        feedforward_weights, feedforward_grad, feedforward_moments, decay_rate
    )
    vector_new, vector_state = adamw_update(norm_vectors, vector_grad, vector_moments, 0.0)
    return (
        from_order(result)[None],
        from_order(grad_stream)[None],
        attention_grad,
        feedforward_grad,
        vector_grad,
        attention_new,
        feedforward_new,
        vector_new,
        attention_state,
        feedforward_state,
        vector_state,
    )


def solution(mesh):
    in_specs = (
        P("fsdp", "seq", None),
        P("fsdp", None),
        P(("seq", "fsdp"), None),
        P(("seq", "fsdp"), None),
        P(None, ("seq", "fsdp")),
        P(None, ("seq", "fsdp"), None),
        P(None, ("seq", "fsdp"), None),
        P(None, None, ("seq", "fsdp")),
        P("fsdp", "seq", None),
    )
    out_specs = (
        P("fsdp", "seq", None),
        P("fsdp", "seq", None),
        P(("seq", "fsdp"), None),
        P(("seq", "fsdp"), None),
        P(None, ("seq", "fsdp")),
        P(("seq", "fsdp"), None),
        P(("seq", "fsdp"), None),
        P(None, ("seq", "fsdp")),
        P(None, ("seq", "fsdp"), None),
        P(None, ("seq", "fsdp"), None),
        P(None, None, ("seq", "fsdp")),
    )
    return jax.shard_map(body, mesh=mesh, in_specs=in_specs, out_specs=out_specs, check_vma=False)
```

```python
import itertools

import jax
import jax.numpy as jnp
from jax import lax
from jax.experimental import pallas as pl
from jax.experimental.pallas import tpu as pltpu
from jax.sharding import PartitionSpec as P

D = 2048
H = 32
HD = 64
ROT = 16
FF = 5632

norm_epsilon = 1e-05
rope_base = 10000.0
neg_fill = -1e30
learn_rate = 0.01
beta_first = 0.9
beta_second = 0.95
adam_epsilon = 1e-08
decay_rate = 0.1
adam_step = 2.0

MESH_IDS = pl.DeviceIdType.MESH
bf16 = jnp.bfloat16
f32 = jnp.float32


def document_positions(segment_ids):
    length = segment_ids.shape[0]
    indices = jnp.arange(length, dtype=jnp.int32)
    changes = jnp.concatenate(
        [jnp.ones((1,), dtype=jnp.bool_), segment_ids[1:] != segment_ids[:-1]]
    )
    starts = lax.cummax(jnp.where(changes, indices, jnp.zeros_like(indices)), axis=0)
    return indices - starts


def rotary_tables(positions, half_rot):
    powers = jnp.arange(half_rot, dtype=jnp.float32) / float(half_rot)
    inverse = rope_base ** (-powers)
    angles = positions.astype(jnp.float32)[:, None] * inverse[None, :]
    return (jnp.cos(angles), jnp.sin(angles))


def rotate(values, cosine, sine, half_rot, direction):
    first = values[..., :half_rot]
    second = values[..., half_rot : 2 * half_rot]
    cosine_wide = cosine[:, None, :]
    sine_wide = sine[:, None, :] * direction
    return jnp.concatenate(
        [
            first * cosine_wide - second * sine_wide,
            second * cosine_wide + first * sine_wide,
            values[..., 2 * half_rot :],
        ],
        axis=-1,
    )


def norm_forward(values, gain, shift):
    centred = values - jnp.mean(values, axis=-1, keepdims=True)
    inverse = lax.rsqrt(jnp.mean(centred * centred, axis=-1, keepdims=True) + norm_epsilon)
    normal_part = centred * inverse
    return (normal_part * gain + shift, normal_part, inverse)


def norm_backward(upstream, normal_part, inverse, gain):
    scaled = upstream * gain
    return inverse * (
        scaled
        - jnp.mean(scaled, axis=-1, keepdims=True)
        - normal_part * jnp.mean(scaled * normal_part, axis=-1, keepdims=True)
    )


def contract_rows(left, right, out=jnp.float32):
    return lax.dot_general(left, right, (((0,), (0,)), ((), ())), preferred_element_type=out)


def contract_cols(left, right, out=jnp.float32):
    return lax.dot_general(left, right, (((1,), (1,)), ((), ())), preferred_element_type=out)


def block_mask(segment_ids, start_row, block_rows):
    total_keys = segment_ids.shape[0]
    row_ids = start_row + jnp.arange(block_rows, dtype=jnp.int32)
    col_ids = jnp.arange(total_keys, dtype=jnp.int32)
    row_segments = lax.dynamic_slice_in_dim(segment_ids, start_row, block_rows)
    return (col_ids[None, :] <= row_ids[:, None]) & (segment_ids[None, :] == row_segments[:, None])


def adamw_update(weight, grad, moments, decay):
    first = beta_first * moments[0] + (1.0 - beta_first) * grad
    second = beta_second * moments[1] + (1.0 - beta_second) * grad * grad
    correct_one = 1.0 - beta_first**adam_step
    correct_two = 1.0 - beta_second**adam_step
    update = first / correct_one / (jnp.sqrt(second / correct_two) + adam_epsilon)
    return (weight - learn_rate * (update + decay * weight), jnp.stack([first, second]))


BOTH = ("seq", "fsdp")


def device_number(y, x, core, z_hi, z_lo):
    return (y * 4 + x * 2 + core) * 4 + z_hi * 2 + z_lo


PLACES = tuple(itertools.product(range(2), repeat=5))
X_FLIP = tuple((device_number(y, x, c, h, l), device_number(y, 1 - x, c, h, l)) for y, x, c, h, l in PLACES)
Z_FLIP = tuple((device_number(y, x, c, h, l), device_number(y, x, c, 1 - h, l)) for y, x, c, h, l in PLACES)
X_Z_SWAP = tuple((device_number(y, x, c, h, l), device_number(y, l, c, h, x)) for y, x, c, h, l in PLACES)
TENSOR_GROUPS = [
    [device_number(y, x, c, h, l) for y in range(2) for l in range(2) for c in range(2)]
    for x in range(2)
    for h in range(2)
]


def head_route(k_x, k_z, back):
    pairs = tuple(
        (device_number(y, x, c, h, l), device_number(y, l ^ k_x, c, h ^ k_z, x))
        for y, x, c, h, l in PLACES
    )
    return tuple((b, a) for a, b in pairs) if back else pairs


def grid_places():
    seq = lax.axis_index("seq")
    fsdp = lax.axis_index("fsdp")
    y, x, core = seq // 4, (seq // 2) % 2, seq % 2
    z_hi, z_lo = fsdp // 2, fsdp % 2
    return seq, fsdp, y, x, core, z_hi, z_lo


def tensor_places():
    seq, fsdp, y, x, core, z_hi, z_lo = grid_places()
    me = y * 4 + z_lo * 2 + core
    step_y = 1 - 2 * y
    step_z = 1 - 2 * z_lo
    step_core = 1 - 2 * core
    sibling = {"seq": seq + step_core, "fsdp": fsdp}
    near = {"seq": seq + core * 4 * step_y, "fsdp": fsdp + (1 - core) * step_z}
    far = {"seq": seq + (1 - core) * 4 * step_y, "fsdp": fsdp + core * step_z}
    near_rank = me + core * 4 * step_y + (1 - core) * 2 * step_z
    far_rank = me + (1 - core) * 4 * step_y + core * 2 * step_z
    corner_rank = near_rank + far_rank - me
    return (me, near_rank, far_rank, corner_rank, step_core), (sibling, near, far)


def greet(others):
    barrier = pltpu.get_barrier_semaphore()
    for other in others:
        pl.semaphore_signal(barrier, inc=1, device_id=other, device_id_type=MESH_IDS)
    pl.semaphore_wait(barrier, len(others))


def gather_kernel(x_ref, o_ref, local_sem, send_sem, recv_sem):
    (me, near_rank, far_rank, corner_rank, _), (sibling, near, far) = tensor_places()

    def copy(source, slot, index, target):
        return pltpu.make_async_remote_copy(
            src_ref=source,
            dst_ref=o_ref.at[slot],
            send_sem=send_sem.at[index],
            recv_sem=recv_sem.at[index],
            device_id=target,
            device_id_type=MESH_IDS,
        )

    greet((sibling, near, far))
    own = pltpu.make_async_copy(x_ref, o_ref.at[me], local_sem)
    own.start()
    to_near = copy(x_ref, me, 0, near)
    to_far = copy(x_ref, me, 1, far)
    to_sibling = copy(x_ref, me, 2, sibling)
    to_near.start()
    to_far.start()
    to_sibling.start()
    to_near.wait_recv()
    near_far = copy(o_ref.at[near_rank], near_rank, 3, far)
    near_far.start()
    near_sibling = copy(o_ref.at[near_rank], near_rank, 4, sibling)
    near_sibling.start()
    to_far.wait_recv()
    far_sibling = copy(o_ref.at[far_rank], far_rank, 5, sibling)
    far_sibling.start()
    near_far.wait_recv()
    corner_sibling = copy(o_ref.at[corner_rank], corner_rank, 6, sibling)
    corner_sibling.start()
    for one in (to_sibling, near_sibling, far_sibling, corner_sibling):
        one.wait_recv()
    for one in (to_near, to_far, to_sibling, near_far, near_sibling, far_sibling, corner_sibling):
        one.wait_send()
    own.wait()


def plane_gather(values, collective_id):
    rows, cols = values.shape
    out = pl.pallas_call(
        gather_kernel,
        out_shape=jax.ShapeDtypeStruct((8, rows, cols), values.dtype),
        in_specs=[pl.BlockSpec(memory_space=pltpu.VMEM)],
        out_specs=pl.BlockSpec(memory_space=pl.ANY),
        scratch_shapes=[
            pltpu.SemaphoreType.DMA,
            pltpu.SemaphoreType.DMA((7,)),
            pltpu.SemaphoreType.DMA((7,)),
        ],
        compiler_params=pltpu.CompilerParams(collective_id=collective_id, has_side_effects=True),
        name="plane_gather",
    )(values)
    return out.reshape(8 * rows, cols)


def scatter_kernel(p_ref, o_ref, mine, pair, near_out, near_in, far_out, far_in, local_sem, send_sem, recv_sem):
    (me, near_rank, far_rank, corner_rank, flip), (sibling, near, far) = tensor_places()
    order = (corner_rank, near_rank, far_rank, me)
    sibling_order = (corner_rank, far_rank, near_rank, me)

    def copy(source, target_ref, index, target):
        return pltpu.make_async_remote_copy(
            src_ref=source,
            dst_ref=target_ref,
            send_sem=send_sem.at[index],
            recv_sem=recv_sem.at[index],
            device_id=target,
            device_id_type=MESH_IDS,
        )

    greet((sibling, near, far))
    pairs = []
    locals_ = []
    for index, block in enumerate(order):
        one = copy(p_ref.at[sibling_order[index] + flip], pair.at[index], index, sibling)
        one.start()
        pairs.append(one)
        own = pltpu.make_async_copy(p_ref.at[block], mine.at[index], local_sem.at[index])
        own.start()
        locals_.append(own)
    for index in range(2):
        pairs[index].wait_recv()
        locals_[index].wait()
        near_out[index] = (mine[index].astype(f32) + pair[index].astype(f32)).astype(near_out.dtype)
        step = copy(near_out.at[index], near_in.at[index], 4 + index, near)
        step.start()
        pairs.append(step)
    for index in range(2, 4):
        pairs[index].wait_recv()
        locals_[index].wait()
    pairs[4].wait_recv()
    far_out[...] = (
        mine[2].astype(f32) + pair[2].astype(f32) + near_in[0].astype(f32)
    ).astype(far_out.dtype)
    last = copy(far_out, far_in, 6, far)
    last.start()
    pairs[5].wait_recv()
    o_ref[...] = mine[3].astype(f32) + pair[3].astype(f32) + near_in[1].astype(f32)
    last.wait_recv()
    o_ref[...] += far_in[...].astype(f32)
    for one in pairs:
        one.wait_send()
    last.wait_send()


def plane_scatter(values, collective_id):
    rows, cols = values.shape
    rows = rows // 8
    return pl.pallas_call(
        scatter_kernel,
        out_shape=jax.ShapeDtypeStruct((rows, cols), f32),
        in_specs=[pl.BlockSpec(memory_space=pl.ANY)],
        out_specs=pl.BlockSpec(memory_space=pltpu.VMEM),
        scratch_shapes=[
            pltpu.VMEM((4, rows, cols), values.dtype),
            pltpu.VMEM((4, rows, cols), values.dtype),
            pltpu.VMEM((2, rows, cols), values.dtype),
            pltpu.VMEM((2, rows, cols), values.dtype),
            pltpu.VMEM((rows, cols), values.dtype),
            pltpu.VMEM((rows, cols), values.dtype),
            pltpu.SemaphoreType.DMA((4,)),
            pltpu.SemaphoreType.DMA((7,)),
            pltpu.SemaphoreType.DMA((7,)),
        ],
        compiler_params=pltpu.CompilerParams(
            collective_id=collective_id, has_side_effects=True, vmem_limit_bytes=32 << 20
        ),
        name="plane_scatter",
    )(values.reshape(8, rows, cols))


def peers(axis, size):
    me = lax.axis_index(axis)
    others = tuple((me + k) % size for k in range(1, size))
    return me, others


def vector_gather_kernel(x_ref, o_ref, send_sem, recv_sem):
    seq, seq_others = peers("seq", 8)
    fsdp, fsdp_others = peers("fsdp", 4)
    greet([{"fsdp": other} for other in fsdp_others] + [{"seq": other} for other in seq_others])
    o_ref[seq, fsdp] = x_ref[...]
    copies = []
    for k, other in enumerate(fsdp_others):
        copies.append(
            pltpu.make_async_remote_copy(
                src_ref=x_ref,
                dst_ref=o_ref.at[seq, fsdp],
                send_sem=send_sem.at[k],
                recv_sem=recv_sem.at[k],
                device_id={"fsdp": other},
                device_id_type=MESH_IDS,
            )
        )
        copies[-1].start()
    for one in copies:
        one.wait_recv()
    for k, other in enumerate(seq_others):
        copies.append(
            pltpu.make_async_remote_copy(
                src_ref=o_ref.at[seq],
                dst_ref=o_ref.at[seq],
                send_sem=send_sem.at[3 + k],
                recv_sem=recv_sem.at[3 + k],
                device_id={"seq": other},
                device_id_type=MESH_IDS,
            )
        )
        copies[-1].start()
    for one in copies[3:]:
        one.wait_recv()
    for one in copies:
        one.wait_send()


def vector_sum_kernel(x_ref, o_ref, part, total, last, send_sem, recv_sem):
    seq, seq_others = peers("seq", 8)
    fsdp, fsdp_others = peers("fsdp", 4)
    greet([{"fsdp": other} for other in fsdp_others] + [{"seq": other} for other in seq_others])
    copies = []
    for k, other in enumerate(seq_others):
        copies.append(
            pltpu.make_async_remote_copy(
                src_ref=x_ref.at[other],
                dst_ref=part.at[k],
                send_sem=send_sem.at[k],
                recv_sem=recv_sem.at[k],
                device_id={"seq": other},
                device_id_type=MESH_IDS,
            )
        )
        copies[-1].start()
    for one in copies:
        one.wait_recv()
    total[...] = x_ref[seq] + jnp.sum(part[...], axis=0)
    for k, other in enumerate(fsdp_others):
        copies.append(
            pltpu.make_async_remote_copy(
                src_ref=total,
                dst_ref=last.at[k],
                send_sem=send_sem.at[7 + k],
                recv_sem=recv_sem.at[7 + k],
                device_id={"fsdp": other},
                device_id_type=MESH_IDS,
            )
        )
        copies[-1].start()
    for one in copies[7:]:
        one.wait_recv()
    o_ref[...] = total[...] + jnp.sum(last[...], axis=0)
    for one in copies:
        one.wait_send()


def gather_vectors(values, collective_id):
    rows = values.shape[1]
    if on_grid():
        padded = jnp.pad(values.astype(f32), ((0, 1), (0, 128 - rows)))
        out = pl.pallas_call(
            vector_gather_kernel,
            out_shape=jax.ShapeDtypeStruct((8, 4, 8, 128), f32),
            in_specs=[pl.BlockSpec(memory_space=pltpu.VMEM)],
            out_specs=pl.BlockSpec(memory_space=pltpu.VMEM),
            scratch_shapes=[pltpu.SemaphoreType.DMA((10,)), pltpu.SemaphoreType.DMA((10,))],
            compiler_params=pltpu.CompilerParams(collective_id=collective_id, has_side_effects=True),
            name="vector_gather",
        )(padded)
        return out[:, :, :7, :rows].transpose(2, 0, 1, 3).reshape(7, D)
    return lax.all_gather(values, BOTH, axis=1, tiled=True).astype(f32)


def sum_vectors(values, collective_id):
    if on_grid():
        blocks = jnp.pad(values.reshape(7, 8, D // 8).transpose(1, 0, 2), ((0, 0), (0, 1), (0, 0)))
        out = pl.pallas_call(
            vector_sum_kernel,
            out_shape=jax.ShapeDtypeStruct((8, D // 8), f32),
            in_specs=[pl.BlockSpec(memory_space=pltpu.VMEM)],
            out_specs=pl.BlockSpec(memory_space=pltpu.VMEM),
            scratch_shapes=[
                pltpu.VMEM((7, 8, D // 8), f32),
                pltpu.VMEM((8, D // 8), f32),
                pltpu.VMEM((3, 8, D // 8), f32),
                pltpu.SemaphoreType.DMA((10,)),
                pltpu.SemaphoreType.DMA((10,)),
            ],
            compiler_params=pltpu.CompilerParams(collective_id=collective_id, has_side_effects=True),
            name="vector_sum",
        )(blocks)
        rows = D // 32
        return lax.dynamic_slice_in_dim(out[:7], lax.axis_index("fsdp") * rows, rows, axis=1)
    return lax.psum_scatter(values, BOTH, scatter_dimension=1, tiled=True)


def on_grid():
    return lax.axis_size("seq") == 8 and lax.axis_size("fsdp") == 4


def after(values, *others):
    return lax.optimization_barrier((values, *others))[0]


class GridPlan:
    def __init__(self, owned_rows):
        _, _, y, self.x, core, self.z_hi, z_lo = grid_places()
        self.rank = y * 4 + z_lo * 2 + core
        self.rows = owned_rows

    def flips(self, values, x_axis, z_axis):
        values = jnp.where(self.x == 1, jnp.flip(values, x_axis), values)
        return jnp.where(self.z_hi == 1, jnp.flip(values, z_axis), values)

    def swap(self, values):
        return lax.ppermute(values, BOTH, X_Z_SWAP)

    def to_order(self, values):
        lead = values.shape[:-1]
        n = len(lead)
        split = values.reshape(*lead, 2, 2, 2, 2, 2, self.rows)
        split = split.transpose(*range(n), n + 1, n + 3, n, n + 4, n + 2, n + 5)
        return self.flips(split, n, n + 1).reshape(*lead, D)

    def from_order(self, values):
        lead = values.shape[:-1]
        n = len(lead)
        split = self.flips(values.reshape(*lead, 2, 2, 2, 2, 2, self.rows), n, n + 1)
        split = split.transpose(*range(n), n + 2, n, n + 4, n + 1, n + 3, n + 5)
        return split.reshape(*lead, D)

    def exchange(self, blocks):
        return lax.all_to_all(
            blocks, BOTH, split_axis=0, concat_axis=0, tiled=True, axis_index_groups=TENSOR_GROUPS
        )

    def gather_rows(self, values):
        over_z = lax.ppermute(values, BOTH, Z_FLIP)
        over_x = lax.ppermute(values, BOTH, X_FLIP)
        over_both = lax.ppermute(over_z, BOTH, X_FLIP)
        return jnp.concatenate([values, over_z, over_x, over_both]), over_z

    def reduce_rows(self, term):
        half = term.shape[0] // 2
        quarter = half // 2
        received = lax.ppermute(term[half:].astype(bf16), BOTH, X_FLIP).astype(f32)
        other = (term[quarter:half] + received[quarter:]).astype(bf16)
        return term[:quarter] + received[:quarter] + lax.ppermute(other, BOTH, Z_FLIP).astype(f32)

    def gather_heads(self, values):
        blocks = [lax.ppermute(values, BOTH, head_route(i, j, False)) for j in range(2) for i in range(2)]
        stacked = jnp.stack(blocks).reshape(2, 2, *values.shape)
        return self.to_order(self.flips(stacked, 1, 0).reshape(-1, D))

    def reduce_heads(self, term):
        blocks = self.from_order(term).reshape(2, 2, -1, D)
        blocks = self.flips(blocks, 1, 0)
        own = [
            lax.ppermute(blocks[j, i].astype(bf16), BOTH, head_route(i, j, True)).astype(f32)
            for j in range(2)
            for i in range(2)
        ]
        return own[0] + own[1] + own[2] + own[3]

    def gather_tokens(self, values, collective_id):
        return plane_gather(values, collective_id)

    def scatter_tokens(self, values, collective_id):
        return plane_scatter(values.astype(bf16), collective_id)


class AxisPlan:
    def __init__(self, owned_rows):
        self.rank = lax.axis_index("seq")
        self.rows = owned_rows
        self.groups = lax.axis_size("seq")
        self.shards = lax.axis_size("fsdp")

    def swap(self, values):
        return values

    def to_order(self, values):
        lead = values.shape[:-1]
        split = values.reshape(*lead, self.groups, self.shards, self.rows)
        return split.swapaxes(-3, -2).reshape(*lead, D)

    def from_order(self, values):
        lead = values.shape[:-1]
        split = values.reshape(*lead, self.shards, self.groups, self.rows)
        return split.swapaxes(-3, -2).reshape(*lead, D)

    def exchange(self, blocks):
        return lax.all_to_all(blocks, "seq", split_axis=0, concat_axis=0, tiled=True)

    def gather_rows(self, values):
        return lax.all_gather(values, "fsdp", axis=0, tiled=True), values

    def reduce_rows(self, term):
        return lax.psum_scatter(term, "fsdp", scatter_dimension=0, tiled=True)

    def gather_heads(self, values):
        return self.to_order(lax.all_gather(values, "fsdp", axis=0, tiled=True))

    def reduce_heads(self, term):
        return self.from_order(lax.psum_scatter(term, "fsdp", scatter_dimension=0, tiled=True))

    def gather_tokens(self, values, collective_id):
        return lax.all_gather(values, "seq", axis=0, tiled=True)

    def scatter_tokens(self, values, collective_id):
        return lax.psum_scatter(values, "seq", scatter_dimension=0, tiled=True)


def body(
    stream,
    segments,
    attention_weights,
    feedforward_weights,
    norm_vectors,
    attention_moments,
    feedforward_moments,
    vector_moments,
    cotangent,
):
    groups = lax.axis_size("seq")
    shards = lax.axis_size("fsdp")
    tokens = stream.shape[1]
    length = tokens * groups
    local_heads = H // groups
    local_width = local_heads * HD
    unit_width = FF // groups
    owned_rows = D // (groups * shards)
    plane_rows = groups * owned_rows
    half_rot = ROT // 2
    score_scale = float(HD) ** (-0.5)
    block_rows = min(512, length)
    block_starts = jnp.arange(length // block_rows, dtype=jnp.int32) * block_rows

    plan = (GridPlan if on_grid() else AxisPlan)(owned_rows)
    my_rank = plan.rank
    to_order, from_order = plan.to_order, plan.from_order

    def spread_columns(values, parts, width):
        blocks = values.reshape(owned_rows, parts, groups, width).transpose(2, 0, 1, 3)
        moved = plan.exchange(blocks.reshape(groups, owned_rows, parts * width))
        return moved.reshape(plane_rows, parts * width)

    vector_full = gather_vectors(norm_vectors.astype(bf16), 9)
    attention_low = attention_weights.astype(bf16)
    feedforward_low = feedforward_weights.astype(bf16)
    qkv_weights, mark = plan.gather_rows(spread_columns(attention_low[:, : 3 * D], 3, local_width))
    out_weights = plan.gather_heads(attention_low[:, 3 * D :])
    in_block = after(spread_columns(feedforward_low[:, : 2 * FF], 2, unit_width), mark)
    in_weights, mark = plan.gather_rows(in_block)
    down_block = after(spread_columns(feedforward_low[:, 2 * FF :], 1, unit_width), mark)
    down_weights, mark = plan.gather_rows(down_block)

    ordered = to_order(vector_full)
    gain_one, shift_one, gain_two, shift_two = [ordered[i] for i in (0, 1, 5, 6)]
    bias = lax.dynamic_slice_in_dim(
        vector_full[2:5], my_rank * local_width, local_width, axis=1
    ).reshape(3 * local_width)
    segment_ids = plan.swap(segments[0])
    cosine, sine = rotary_tables(document_positions(segment_ids), half_rot)

    inputs = to_order(plan.swap(stream[0]))
    upstream = to_order(plan.swap(cotangent[0]))
    normed_one, normal_one, inverse_one = norm_forward(inputs, gain_one, shift_one)
    normed_all = plan.gather_tokens(normed_one.astype(bf16), 1)
    cotangent_all = plan.gather_tokens(upstream.astype(bf16), 2)
    projected = (
        jnp.dot(normed_all, qkv_weights, preferred_element_type=f32) + bias
    ).reshape(length, 3, local_heads, HD)
    query_all = rotate(projected[:, 0], cosine, sine, half_rot, 1.0).astype(bf16)
    key_all = rotate(projected[:, 1], cosine, sine, half_rot, 1.0).astype(bf16)
    value_all = projected[:, 2].astype(bf16)

    def forward_block(start_row):
        query_block = lax.dynamic_slice_in_dim(query_all, start_row, block_rows)
        scores = (
            jnp.einsum("bhd,lhd->hbl", query_block, key_all, preferred_element_type=jnp.float32)
            * score_scale
        )
        scores = jnp.where(block_mask(segment_ids, start_row, block_rows)[None], scores, neg_fill)
        row_max = jnp.max(scores, axis=-1, keepdims=True)
        weights_raw = jnp.exp(scores - row_max)
        row_sum = jnp.sum(weights_raw, axis=-1, keepdims=True)
        probability = (weights_raw / row_sum).astype(jnp.bfloat16)
        output_block = jnp.einsum(
            "hbl,lhd->bhd", probability, value_all, preferred_element_type=jnp.float32
        ).astype(jnp.bfloat16)
        return (output_block, (row_max + jnp.log(row_sum))[..., 0])

    output_blocks, logsum_blocks = lax.map(forward_block, block_starts)
    output_heads = output_blocks.reshape(length, local_heads, HD)
    attended = output_heads.reshape(length, local_width)
    hidden = inputs + plan.scatter_tokens(jnp.dot(attended, out_weights, preferred_element_type=f32), 3)
    normed_two, normal_two, inverse_two = norm_forward(hidden, gain_two, shift_two)
    normed_two_all = plan.gather_tokens(normed_two.astype(bf16), 4)
    gate_up = jnp.dot(normed_two_all, in_weights, preferred_element_type=f32)
    gate_part = gate_up[:, :unit_width]
    up_part = gate_up[:, unit_width:]
    sigmoid_gate = jax.nn.sigmoid(gate_part)
    activated = (gate_part * sigmoid_gate * up_part).astype(bf16)
    grad_act = jnp.dot(cotangent_all, down_weights, preferred_element_type=f32)
    grad_gate = grad_act * up_part * sigmoid_gate * (1.0 + gate_part * (1.0 - sigmoid_gate))
    grad_up = grad_act * gate_part * sigmoid_gate
    grad_gate_up = jnp.concatenate([grad_gate, grad_up], axis=1).astype(bf16)
    grad_normed_two = plan.scatter_tokens(contract_cols(grad_gate_up, in_weights), 5)

    def collect_rows(total, parts, width):
        moved = plan.exchange(total.astype(bf16).reshape(groups, owned_rows, parts * width))
        moved = moved.astype(f32).reshape(groups, owned_rows, parts, width)
        return moved.transpose(1, 2, 0, 3).reshape(owned_rows, parts * groups * width)

    down_sum = plan.reduce_rows(contract_rows(cotangent_all, activated))
    in_sum = plan.reduce_rows(contract_rows(normed_two_all, grad_gate_up))

    grad_hidden = upstream + norm_backward(grad_normed_two, normal_two, inverse_two, gain_two)
    grad_gain_two = jnp.sum(grad_normed_two * normal_two, axis=0)
    grad_shift_two = jnp.sum(grad_normed_two, axis=0)
    grad_hidden_all = plan.gather_tokens(grad_hidden.astype(bf16), 6)
    grad_heads = (
        contract_cols(grad_hidden_all, out_weights).astype(bf16).reshape(length, local_heads, HD)
    )
    out_sum = plan.reduce_heads(contract_rows(attended, grad_hidden_all))
    result = hidden + plan.scatter_tokens(contract_cols(activated, down_weights), 7)

    def backward_block(carry, items):
        grad_key_sum, grad_value_sum = carry
        start_row, logsum_block = items
        query_block = lax.dynamic_slice_in_dim(query_all, start_row, block_rows)
        output_block = lax.dynamic_slice_in_dim(output_heads, start_row, block_rows)
        grad_block = lax.dynamic_slice_in_dim(grad_heads, start_row, block_rows)
        scores = (
            jnp.einsum("bhd,lhd->hbl", query_block, key_all, preferred_element_type=jnp.float32)
            * score_scale
        )
        scores = jnp.where(block_mask(segment_ids, start_row, block_rows)[None], scores, neg_fill)
        probability = jnp.exp(scores - logsum_block[..., None])
        prob_low = probability.astype(jnp.bfloat16)
        grad_value_sum = grad_value_sum + jnp.einsum(
            "hbl,bhd->lhd", prob_low, grad_block, preferred_element_type=jnp.float32
        )
        grad_prob = jnp.einsum(
            "bhd,lhd->hbl", grad_block, value_all, preferred_element_type=jnp.float32
        )
        row_delta = jnp.sum(
            grad_block.astype(jnp.float32) * output_block.astype(jnp.float32), axis=-1
        )
        row_delta = jnp.transpose(row_delta)[..., None]
        grad_scores = (probability * (grad_prob - row_delta) * score_scale).astype(jnp.bfloat16)
        grad_query = jnp.einsum(
            "hbl,lhd->bhd", grad_scores, key_all, preferred_element_type=jnp.float32
        ).astype(jnp.bfloat16)
        grad_key_sum = grad_key_sum + jnp.einsum(
            "hbl,bhd->lhd", grad_scores, query_block, preferred_element_type=jnp.float32
        )
        return ((grad_key_sum, grad_value_sum), grad_query)

    zero_heads = jnp.zeros((length, local_heads, HD), jnp.float32)
    sums, grad_query_blocks = lax.scan(
        backward_block, (zero_heads, zero_heads), (block_starts, logsum_blocks)
    )
    grad_key_sum, grad_value_sum = sums
    grad_query_low = grad_query_blocks.reshape(length, local_heads, HD)
    grad_projected = jnp.concatenate(
        [
            rotate(grad_query_low.astype(f32), cosine, sine, half_rot, -1.0).reshape(
                length, local_width
            ),
            rotate(
                lax.optimization_barrier(grad_key_sum.astype(bf16)).astype(f32),
                cosine,
                sine,
                half_rot,
                -1.0,
            ).reshape(length, local_width),
            lax.optimization_barrier(grad_value_sum.astype(bf16)).astype(f32).reshape(
                length, local_width
            ),
        ],
        axis=1,
    )
    grad_bias = jnp.sum(grad_projected, axis=0)
    grad_projected_low = grad_projected.astype(bf16)
    qkv_sum = plan.reduce_rows(contract_rows(normed_all, grad_projected_low))
    grad_normed_one = plan.scatter_tokens(contract_cols(grad_projected_low, qkv_weights), 8)
    grad_stream = grad_hidden + norm_backward(grad_normed_one, normal_one, inverse_one, gain_one)
    grad_gain_one = jnp.sum(grad_normed_one * normal_one, axis=0)
    grad_shift_one = jnp.sum(grad_normed_one, axis=0)

    feedforward_grad = jnp.concatenate(
        [collect_rows(in_sum, 2, unit_width), collect_rows(down_sum, 1, unit_width)], axis=1
    )
    attention_grad = jnp.concatenate(
        [collect_rows(qkv_sum, 3, local_width), out_sum], axis=1
    )
    bias_rows = lax.dynamic_update_slice_in_dim(
        jnp.zeros((3, D), f32), grad_bias.reshape(3, local_width), my_rank * local_width, axis=1
    )
    vector_term = jnp.concatenate(
        [
            from_order(jnp.stack([grad_gain_one, grad_shift_one])),
            bias_rows,
            from_order(jnp.stack([grad_gain_two, grad_shift_two])),
        ]
    )
    vector_grad = sum_vectors(vector_term, 10)
    attention_new, attention_state = adamw_update(
        attention_weights, attention_grad, attention_moments, decay_rate
    )
    feedforward_new, feedforward_state = adamw_update(
        feedforward_weights, feedforward_grad, feedforward_moments, decay_rate
    )
    vector_new, vector_state = adamw_update(norm_vectors, vector_grad, vector_moments, 0.0)
    return (
        plan.swap(from_order(result))[None],
        plan.swap(from_order(grad_stream))[None],
        attention_grad,
        feedforward_grad,
        vector_grad,
        attention_new,
        feedforward_new,
        vector_new,
        attention_state,
        feedforward_state,
        vector_state,
    )


def solution(mesh):
    in_specs = (
        P("fsdp", "seq", None),
        P("fsdp", None),
        P(("seq", "fsdp"), None),
        P(("seq", "fsdp"), None),
        P(None, ("seq", "fsdp")),
        P(None, ("seq", "fsdp"), None),
        P(None, ("seq", "fsdp"), None),
        P(None, None, ("seq", "fsdp")),
        P("fsdp", "seq", None),
    )
    out_specs = (
        P("fsdp", "seq", None),
        P("fsdp", "seq", None),
        P(("seq", "fsdp"), None),
        P(("seq", "fsdp"), None),
        P(None, ("seq", "fsdp")),
        P(("seq", "fsdp"), None),
        P(("seq", "fsdp"), None),
        P(None, ("seq", "fsdp")),
        P(None, ("seq", "fsdp"), None),
        P(None, ("seq", "fsdp"), None),
        P(None, None, ("seq", "fsdp")),
    )
    return jax.shard_map(body, mesh=mesh, in_specs=in_specs, out_specs=out_specs, check_vma=False)
```

```python
import jax
import jax.numpy as jnp
from jax import lax
from jax.experimental import pallas as pl
from jax.experimental.pallas import tpu as pltpu
from jax.sharding import PartitionSpec as P

D = 2048
H = 32
HD = 64
ROT = 16
FF = 5632

norm_epsilon = 1e-05
rope_base = 10000.0
neg_fill = -1e30
learn_rate = 0.01
beta_first = 0.9
beta_second = 0.95
adam_epsilon = 1e-08
decay_rate = 0.1
adam_step = 2.0

MESH_IDS = pl.DeviceIdType.MESH
BOTH = ("seq", "fsdp")
bf16 = jnp.bfloat16
f32 = jnp.float32


def document_positions(segment_ids):
    length = segment_ids.shape[0]
    indices = jnp.arange(length, dtype=jnp.int32)
    changes = jnp.concatenate(
        [jnp.ones((1,), dtype=jnp.bool_), segment_ids[1:] != segment_ids[:-1]]
    )
    starts = lax.cummax(jnp.where(changes, indices, jnp.zeros_like(indices)), axis=0)
    return indices - starts


def rotary_tables(positions, half_rot):
    powers = jnp.arange(half_rot, dtype=jnp.float32) / float(half_rot)
    inverse = rope_base ** (-powers)
    angles = positions.astype(jnp.float32)[:, None] * inverse[None, :]
    return (jnp.cos(angles), jnp.sin(angles))


def rotate(values, cosine, sine, half_rot, direction):
    first = values[..., :half_rot]
    second = values[..., half_rot : 2 * half_rot]
    cosine_wide = cosine[:, None, :]
    sine_wide = sine[:, None, :] * direction
    return jnp.concatenate(
        [
            first * cosine_wide - second * sine_wide,
            second * cosine_wide + first * sine_wide,
            values[..., 2 * half_rot :],
        ],
        axis=-1,
    )


def norm_forward(values, gain, shift):
    centred = values - jnp.mean(values, axis=-1, keepdims=True)
    inverse = lax.rsqrt(jnp.mean(centred * centred, axis=-1, keepdims=True) + norm_epsilon)
    normal_part = centred * inverse
    return (normal_part * gain + shift, normal_part, inverse)


def norm_backward(upstream, normal_part, inverse, gain):
    scaled = upstream * gain
    return inverse * (
        scaled
        - jnp.mean(scaled, axis=-1, keepdims=True)
        - normal_part * jnp.mean(scaled * normal_part, axis=-1, keepdims=True)
    )


def contract_rows(left, right, out=jnp.float32):
    return lax.dot_general(left, right, (((0,), (0,)), ((), ())), preferred_element_type=out)


def contract_cols(left, right, out=jnp.float32):
    return lax.dot_general(left, right, (((1,), (1,)), ((), ())), preferred_element_type=out)


def block_mask(segment_ids, start_row, block_rows):
    total_keys = segment_ids.shape[0]
    row_ids = start_row + jnp.arange(block_rows, dtype=jnp.int32)
    col_ids = jnp.arange(total_keys, dtype=jnp.int32)
    row_segments = lax.dynamic_slice_in_dim(segment_ids, start_row, block_rows)
    return (col_ids[None, :] <= row_ids[:, None]) & (segment_ids[None, :] == row_segments[:, None])


def adamw_update(weight, grad, moments, decay):
    first = beta_first * moments[0] + (1.0 - beta_first) * grad
    second = beta_second * moments[1] + (1.0 - beta_second) * grad * grad
    correct_one = 1.0 - beta_first**adam_step
    correct_two = 1.0 - beta_second**adam_step
    update = first / correct_one / (jnp.sqrt(second / correct_two) + adam_epsilon)
    return (weight - learn_rate * (update + decay * weight), jnp.stack([first, second]))


def plane_places():
    me = lax.axis_index("seq")
    core = me % 2
    first = 2 + 2 * core
    second = 4 - 2 * core
    bit_first = (me // first) % 2
    bit_second = (me // second) % 2
    sibling = me + 1 - 2 * core
    near = me + first * (1 - 2 * bit_first)
    far = me + second * (1 - 2 * bit_second)
    corner = near + second * (1 - 2 * bit_second)
    return me, sibling, near, far, corner


def greet(others):
    barrier = pltpu.get_barrier_semaphore()
    for other in others:
        pl.semaphore_signal(barrier, inc=1, device_id=other, device_id_type=MESH_IDS)
    pl.semaphore_wait(barrier, len(others))


def gather_kernel(x_ref, o_ref, local_sem, send_sem, recv_sem):
    me, sibling, near, far, corner = plane_places()

    def copy(source, slot, index, target):
        return pltpu.make_async_remote_copy(
            src_ref=source,
            dst_ref=o_ref.at[slot],
            send_sem=send_sem.at[index],
            recv_sem=recv_sem.at[index],
            device_id={"seq": target},
            device_id_type=MESH_IDS,
        )

    greet([{"seq": other} for other in (sibling, near, far)])
    own = pltpu.make_async_copy(x_ref, o_ref.at[me], local_sem)
    own.start()
    to_near = copy(x_ref, me, 0, near)
    to_far = copy(x_ref, me, 1, far)
    to_sibling = copy(x_ref, me, 2, sibling)
    to_near.start()
    to_far.start()
    to_sibling.start()
    to_near.wait_recv()
    near_far = copy(o_ref.at[near], near, 3, far)
    near_far.start()
    near_sibling = copy(o_ref.at[near], near, 4, sibling)
    near_sibling.start()
    to_far.wait_recv()
    far_sibling = copy(o_ref.at[far], far, 5, sibling)
    far_sibling.start()
    near_far.wait_recv()
    corner_sibling = copy(o_ref.at[corner], corner, 6, sibling)
    corner_sibling.start()
    for one in (to_sibling, near_sibling, far_sibling, corner_sibling):
        one.wait_recv()
    for one in (to_near, to_far, to_sibling, near_far, near_sibling, far_sibling, corner_sibling):
        one.wait_send()
    own.wait()


def plane_gather(values, collective_id):
    rows, cols = values.shape
    out = pl.pallas_call(
        gather_kernel,
        out_shape=jax.ShapeDtypeStruct((8, rows, cols), values.dtype),
        in_specs=[pl.BlockSpec(memory_space=pltpu.VMEM)],
        out_specs=pl.BlockSpec(memory_space=pl.ANY),
        scratch_shapes=[
            pltpu.SemaphoreType.DMA,
            pltpu.SemaphoreType.DMA((7,)),
            pltpu.SemaphoreType.DMA((7,)),
        ],
        compiler_params=pltpu.CompilerParams(collective_id=collective_id, has_side_effects=True),
        name="plane_gather",
    )(values)
    return out.reshape(8 * rows, cols)


def scatter_kernel(p_ref, o_ref, mine, pair, near_out, near_in, far_out, far_in, local_sem, send_sem, recv_sem):
    me, sibling, near, far, corner = plane_places()
    flip = sibling - me
    order = (corner, near, far, me)
    sibling_order = (corner, far, near, me)

    def copy(source, target_ref, index, target):
        return pltpu.make_async_remote_copy(
            src_ref=source,
            dst_ref=target_ref,
            send_sem=send_sem.at[index],
            recv_sem=recv_sem.at[index],
            device_id={"seq": target},
            device_id_type=MESH_IDS,
        )

    greet([{"seq": other} for other in (sibling, near, far)])
    pairs = []
    locals_ = []
    for index, block in enumerate(order):
        one = copy(p_ref.at[sibling_order[index] + flip], pair.at[index], index, sibling)
        one.start()
        pairs.append(one)
        own = pltpu.make_async_copy(p_ref.at[block], mine.at[index], local_sem.at[index])
        own.start()
        locals_.append(own)
    for index in range(2):
        pairs[index].wait_recv()
        locals_[index].wait()
        near_out[index] = (mine[index].astype(f32) + pair[index].astype(f32)).astype(near_out.dtype)
        step = copy(near_out.at[index], near_in.at[index], 4 + index, near)
        step.start()
        pairs.append(step)
    for index in range(2, 4):
        pairs[index].wait_recv()
        locals_[index].wait()
    pairs[4].wait_recv()
    far_out[...] = (
        mine[2].astype(f32) + pair[2].astype(f32) + near_in[0].astype(f32)
    ).astype(far_out.dtype)
    last = copy(far_out, far_in, 6, far)
    last.start()
    pairs[5].wait_recv()
    o_ref[...] = mine[3].astype(f32) + pair[3].astype(f32) + near_in[1].astype(f32)
    last.wait_recv()
    o_ref[...] += far_in[...].astype(f32)
    for one in pairs:
        one.wait_send()
    last.wait_send()


def plane_scatter(values, collective_id):
    rows, cols = values.shape
    rows = rows // 8
    return pl.pallas_call(
        scatter_kernel,
        out_shape=jax.ShapeDtypeStruct((rows, cols), f32),
        in_specs=[pl.BlockSpec(memory_space=pl.ANY)],
        out_specs=pl.BlockSpec(memory_space=pltpu.VMEM),
        scratch_shapes=[
            pltpu.VMEM((4, rows, cols), values.dtype),
            pltpu.VMEM((4, rows, cols), values.dtype),
            pltpu.VMEM((2, rows, cols), values.dtype),
            pltpu.VMEM((2, rows, cols), values.dtype),
            pltpu.VMEM((rows, cols), values.dtype),
            pltpu.VMEM((rows, cols), values.dtype),
            pltpu.SemaphoreType.DMA((4,)),
            pltpu.SemaphoreType.DMA((7,)),
            pltpu.SemaphoreType.DMA((7,)),
        ],
        compiler_params=pltpu.CompilerParams(
            collective_id=collective_id, has_side_effects=True, vmem_limit_bytes=32 << 20
        ),
        name="plane_scatter",
    )(values.reshape(8, rows, cols))


def peers(axis, size):
    me = lax.axis_index(axis)
    others = tuple((me + k) % size for k in range(1, size))
    return me, others


def vector_gather_kernel(x_ref, o_ref, send_sem, recv_sem):
    seq, seq_others = peers("seq", 8)
    fsdp, fsdp_others = peers("fsdp", 4)
    greet([{"fsdp": other} for other in fsdp_others] + [{"seq": other} for other in seq_others])
    o_ref[seq, fsdp] = x_ref[...]
    copies = []
    for k, other in enumerate(fsdp_others):
        copies.append(
            pltpu.make_async_remote_copy(
                src_ref=x_ref,
                dst_ref=o_ref.at[seq, fsdp],
                send_sem=send_sem.at[k],
                recv_sem=recv_sem.at[k],
                device_id={"fsdp": other},
                device_id_type=MESH_IDS,
            )
        )
        copies[-1].start()
    for one in copies:
        one.wait_recv()
    for k, other in enumerate(seq_others):
        copies.append(
            pltpu.make_async_remote_copy(
                src_ref=o_ref.at[seq],
                dst_ref=o_ref.at[seq],
                send_sem=send_sem.at[3 + k],
                recv_sem=recv_sem.at[3 + k],
                device_id={"seq": other},
                device_id_type=MESH_IDS,
            )
        )
        copies[-1].start()
    for one in copies[3:]:
        one.wait_recv()
    for one in copies:
        one.wait_send()


def vector_sum_kernel(x_ref, o_ref, part, total, last, send_sem, recv_sem):
    seq, seq_others = peers("seq", 8)
    _, fsdp_others = peers("fsdp", 4)
    greet([{"fsdp": other} for other in fsdp_others] + [{"seq": other} for other in seq_others])
    copies = []
    for k, other in enumerate(seq_others):
        copies.append(
            pltpu.make_async_remote_copy(
                src_ref=x_ref.at[other],
                dst_ref=part.at[k],
                send_sem=send_sem.at[k],
                recv_sem=recv_sem.at[k],
                device_id={"seq": other},
                device_id_type=MESH_IDS,
            )
        )
        copies[-1].start()
    for one in copies:
        one.wait_recv()
    total[...] = x_ref[seq] + jnp.sum(part[...], axis=0)
    for k, other in enumerate(fsdp_others):
        copies.append(
            pltpu.make_async_remote_copy(
                src_ref=total,
                dst_ref=last.at[k],
                send_sem=send_sem.at[7 + k],
                recv_sem=recv_sem.at[7 + k],
                device_id={"fsdp": other},
                device_id_type=MESH_IDS,
            )
        )
        copies[-1].start()
    for one in copies[7:]:
        one.wait_recv()
    o_ref[...] = total[...] + jnp.sum(last[...], axis=0)
    for one in copies:
        one.wait_send()


def gather_vectors(values, collective_id):
    rows = values.shape[1]
    if on_grid():
        padded = jnp.pad(values.astype(f32), ((0, 1), (0, 128 - rows)))
        out = pl.pallas_call(
            vector_gather_kernel,
            out_shape=jax.ShapeDtypeStruct((8, 4, 8, 128), f32),
            in_specs=[pl.BlockSpec(memory_space=pltpu.VMEM)],
            out_specs=pl.BlockSpec(memory_space=pltpu.VMEM),
            scratch_shapes=[pltpu.SemaphoreType.DMA((10,)), pltpu.SemaphoreType.DMA((10,))],
            compiler_params=pltpu.CompilerParams(collective_id=collective_id, has_side_effects=True),
            name="vector_gather",
        )(padded)
        return out[:, :, :7, :rows].transpose(2, 0, 1, 3).reshape(7, D)
    return lax.all_gather(values, BOTH, axis=1, tiled=True).astype(f32)


def sum_vectors(values, collective_id):
    if on_grid():
        blocks = jnp.pad(values.reshape(7, 8, D // 8).transpose(1, 0, 2), ((0, 0), (0, 1), (0, 0)))
        out = pl.pallas_call(
            vector_sum_kernel,
            out_shape=jax.ShapeDtypeStruct((8, D // 8), f32),
            in_specs=[pl.BlockSpec(memory_space=pltpu.VMEM)],
            out_specs=pl.BlockSpec(memory_space=pltpu.VMEM),
            scratch_shapes=[
                pltpu.VMEM((7, 8, D // 8), f32),
                pltpu.VMEM((8, D // 8), f32),
                pltpu.VMEM((3, 8, D // 8), f32),
                pltpu.SemaphoreType.DMA((10,)),
                pltpu.SemaphoreType.DMA((10,)),
            ],
            compiler_params=pltpu.CompilerParams(collective_id=collective_id, has_side_effects=True),
            name="vector_sum",
        )(blocks)
        rows = D // 32
        return lax.dynamic_slice_in_dim(out[:7], lax.axis_index("fsdp") * rows, rows, axis=1)
    return lax.psum_scatter(values, BOTH, scatter_dimension=1, tiled=True)


def on_grid():
    return lax.axis_size("seq") == 8 and lax.axis_size("fsdp") == 4


def after(values, *others):
    return lax.optimization_barrier((values, *others))[0]


def gather_tokens(values, collective_id):
    if lax.axis_size("seq") == 8:
        return plane_gather(values, collective_id)
    return lax.all_gather(values, "seq", axis=0, tiled=True)


def scatter_tokens(values, collective_id):
    if lax.axis_size("seq") == 8:
        return plane_scatter(values.astype(bf16), collective_id)
    return lax.psum_scatter(values, "seq", scatter_dimension=0, tiled=True)


def body(
    stream,
    segments,
    attention_weights,
    feedforward_weights,
    norm_vectors,
    attention_moments,
    feedforward_moments,
    vector_moments,
    cotangent,
):
    groups = lax.axis_size("seq")
    shards = lax.axis_size("fsdp")
    my_rank = lax.axis_index("seq")
    tokens = stream.shape[1]
    length = tokens * groups
    local_heads = H // groups
    local_width = local_heads * HD
    unit_width = FF // groups
    owned_rows = D // (groups * shards)
    plane_rows = groups * owned_rows
    half_rot = ROT // 2
    score_scale = float(HD) ** (-0.5)
    block_rows = min(512, length)
    block_starts = jnp.arange(length // block_rows, dtype=jnp.int32) * block_rows

    def to_order(values):
        lead = values.shape[:-1]
        return values.reshape(*lead, groups, shards, owned_rows).swapaxes(-3, -2).reshape(*lead, D)

    def from_order(values):
        lead = values.shape[:-1]
        return values.reshape(*lead, shards, groups, owned_rows).swapaxes(-3, -2).reshape(*lead, D)

    def spread_columns(values, parts, width):
        blocks = values.reshape(owned_rows, parts, groups, width).transpose(2, 0, 1, 3)
        blocks = blocks.reshape(groups, owned_rows, parts * width)
        moved = lax.all_to_all(blocks, "seq", split_axis=0, concat_axis=0, tiled=True)
        return moved.reshape(plane_rows, parts * width)

    vector_full = gather_vectors(norm_vectors.astype(bf16), 9)
    attention_low = attention_weights.astype(bf16)
    feedforward_low = feedforward_weights.astype(bf16)
    out_weights = lax.all_gather(attention_low[:, 3 * D :], "fsdp", axis=0, tiled=True)
    out_weights = to_order(out_weights)
    qkv_block = spread_columns(attention_low[:, : 3 * D], 3, local_width)
    qkv_weights = lax.all_gather(qkv_block, "fsdp", axis=0, tiled=True)
    down_block = spread_columns(feedforward_low[:, 2 * FF :], 1, unit_width)
    down_weights = lax.all_gather(down_block, "fsdp", axis=0, tiled=True)
    in_block = spread_columns(feedforward_low[:, : 2 * FF], 2, unit_width)
    in_weights = lax.all_gather(in_block, "fsdp", axis=0, tiled=True)

    ordered = to_order(vector_full)
    gain_one, shift_one, gain_two, shift_two = [ordered[i] for i in (0, 1, 5, 6)]
    bias = lax.dynamic_slice_in_dim(
        vector_full[2:5], my_rank * local_width, local_width, axis=1
    ).reshape(3 * local_width)
    segment_ids = segments[0]
    cosine, sine = rotary_tables(document_positions(segment_ids), half_rot)

    inputs = to_order(stream[0])
    upstream = to_order(cotangent[0])
    normed_one, normal_one, inverse_one = norm_forward(inputs, gain_one, shift_one)
    normed_all = gather_tokens(normed_one.astype(bf16), 1)
    cotangent_all = gather_tokens(upstream.astype(bf16), 2)
    projected = (
        jnp.dot(normed_all, qkv_weights, preferred_element_type=f32) + bias
    ).reshape(length, 3, local_heads, HD)
    query_all = rotate(projected[:, 0], cosine, sine, half_rot, 1.0).astype(bf16)
    key_all = rotate(projected[:, 1], cosine, sine, half_rot, 1.0).astype(bf16)
    value_all = projected[:, 2].astype(bf16)

    def forward_block(start_row):
        query_block = lax.dynamic_slice_in_dim(query_all, start_row, block_rows)
        scores = (
            jnp.einsum("bhd,lhd->hbl", query_block, key_all, preferred_element_type=jnp.float32)
            * score_scale
        )
        scores = jnp.where(block_mask(segment_ids, start_row, block_rows)[None], scores, neg_fill)
        row_max = jnp.max(scores, axis=-1, keepdims=True)
        weights_raw = jnp.exp(scores - row_max)
        row_sum = jnp.sum(weights_raw, axis=-1, keepdims=True)
        probability = (weights_raw / row_sum).astype(jnp.bfloat16)
        output_block = jnp.einsum(
            "hbl,lhd->bhd", probability, value_all, preferred_element_type=jnp.float32
        ).astype(jnp.bfloat16)
        return (output_block, (row_max + jnp.log(row_sum))[..., 0])

    output_blocks, logsum_blocks = lax.map(forward_block, block_starts)
    output_heads = output_blocks.reshape(length, local_heads, HD)
    attended = output_heads.reshape(length, local_width)
    hidden = inputs + scatter_tokens(jnp.dot(attended, out_weights, preferred_element_type=f32), 3)
    normed_two, normal_two, inverse_two = norm_forward(hidden, gain_two, shift_two)
    normed_two_all = gather_tokens(normed_two.astype(bf16), 4)
    grad_act = jnp.dot(cotangent_all, down_weights, preferred_element_type=f32)
    gate_up = jnp.dot(normed_two_all, in_weights, preferred_element_type=f32)
    gate_part = gate_up[:, :unit_width]
    up_part = gate_up[:, unit_width:]
    sigmoid_gate = jax.nn.sigmoid(gate_part)
    activated = (gate_part * sigmoid_gate * up_part).astype(bf16)
    grad_gate = grad_act * up_part * sigmoid_gate * (1.0 + gate_part * (1.0 - sigmoid_gate))
    grad_up = grad_act * gate_part * sigmoid_gate
    grad_gate_up = jnp.concatenate([grad_gate, grad_up], axis=1).astype(bf16)

    def reduce_rows(term):
        return lax.psum_scatter(term, "fsdp", scatter_dimension=0, tiled=True)

    def collect_rows(total, parts, width):
        moved = lax.all_to_all(
            total.reshape(groups, owned_rows, parts, width),
            "seq",
            split_axis=0,
            concat_axis=0,
            tiled=True,
        ).astype(f32)
        return moved.transpose(1, 2, 0, 3).reshape(owned_rows, parts * groups * width)

    down_term = contract_rows(cotangent_all, activated).astype(bf16)
    down_sum = reduce_rows(down_term)
    in_term = contract_rows(normed_two_all, after(grad_gate_up, down_term)).astype(bf16)
    in_sum = reduce_rows(in_term)
    grad_normed_two = scatter_tokens(
        contract_cols(after(grad_gate_up, in_term), in_weights), 5
    )

    grad_hidden = upstream + norm_backward(grad_normed_two, normal_two, inverse_two, gain_two)
    grad_gain_two = jnp.sum(grad_normed_two * normal_two, axis=0)
    grad_shift_two = jnp.sum(grad_normed_two, axis=0)
    grad_hidden_all = gather_tokens(grad_hidden.astype(bf16), 6)
    grad_heads = (
        contract_cols(grad_hidden_all, out_weights).astype(bf16).reshape(length, local_heads, HD)
    )

    def backward_block(carry, items):
        grad_key_sum, grad_value_sum = carry
        start_row, logsum_block = items
        query_block = lax.dynamic_slice_in_dim(query_all, start_row, block_rows)
        output_block = lax.dynamic_slice_in_dim(output_heads, start_row, block_rows)
        grad_block = lax.dynamic_slice_in_dim(grad_heads, start_row, block_rows)
        scores = (
            jnp.einsum("bhd,lhd->hbl", query_block, key_all, preferred_element_type=jnp.float32)
            * score_scale
        )
        scores = jnp.where(block_mask(segment_ids, start_row, block_rows)[None], scores, neg_fill)
        probability = jnp.exp(scores - logsum_block[..., None])
        prob_low = probability.astype(jnp.bfloat16)
        grad_value_sum = grad_value_sum + jnp.einsum(
            "hbl,bhd->lhd", prob_low, grad_block, preferred_element_type=jnp.float32
        )
        grad_prob = jnp.einsum(
            "bhd,lhd->hbl", grad_block, value_all, preferred_element_type=jnp.float32
        )
        row_delta = jnp.sum(
            grad_block.astype(jnp.float32) * output_block.astype(jnp.float32), axis=-1
        )
        row_delta = jnp.transpose(row_delta)[..., None]
        grad_scores = (probability * (grad_prob - row_delta) * score_scale).astype(jnp.bfloat16)
        grad_query = jnp.einsum(
            "hbl,lhd->bhd", grad_scores, key_all, preferred_element_type=jnp.float32
        ).astype(jnp.bfloat16)
        grad_key_sum = grad_key_sum + jnp.einsum(
            "hbl,bhd->lhd", grad_scores, query_block, preferred_element_type=jnp.float32
        )
        return ((grad_key_sum, grad_value_sum), grad_query)

    zero_heads = jnp.zeros((length, local_heads, HD), jnp.float32)
    sums, grad_query_blocks = lax.scan(
        backward_block, (zero_heads, zero_heads), (block_starts, logsum_blocks)
    )
    grad_key_sum, grad_value_sum = sums
    grad_query_low = grad_query_blocks.reshape(length, local_heads, HD)
    grad_projected = jnp.concatenate(
        [
            rotate(grad_query_low.astype(f32), cosine, sine, half_rot, -1.0).reshape(
                length, local_width
            ),
            rotate(
                lax.optimization_barrier(grad_key_sum.astype(bf16)).astype(f32),
                cosine,
                sine,
                half_rot,
                -1.0,
            ).reshape(length, local_width),
            lax.optimization_barrier(grad_value_sum.astype(bf16)).astype(f32).reshape(
                length, local_width
            ),
        ],
        axis=1,
    )
    grad_bias = jnp.sum(grad_projected, axis=0)
    grad_projected_low = grad_projected.astype(bf16)
    qkv_term = contract_rows(normed_all, grad_projected_low).astype(bf16)
    qkv_sum = reduce_rows(qkv_term)
    out_term = contract_rows(attended, after(grad_hidden_all, qkv_term)).astype(bf16)
    out_sum = reduce_rows(out_term)
    grad_normed_one = scatter_tokens(
        contract_cols(after(grad_projected_low, out_term), qkv_weights), 8
    )
    result = hidden + scatter_tokens(
        contract_cols(after(activated, grad_normed_one), down_weights), 7
    )
    grad_stream = grad_hidden + norm_backward(grad_normed_one, normal_one, inverse_one, gain_one)
    grad_gain_one = jnp.sum(grad_normed_one * normal_one, axis=0)
    grad_shift_one = jnp.sum(grad_normed_one, axis=0)

    feedforward_grad = jnp.concatenate(
        [collect_rows(in_sum, 2, unit_width), collect_rows(down_sum, 1, unit_width)], axis=1
    )
    attention_grad = jnp.concatenate(
        [collect_rows(qkv_sum, 3, local_width), from_order(out_sum.astype(f32))], axis=1
    )
    bias_rows = lax.dynamic_update_slice_in_dim(
        jnp.zeros((3, D), f32), grad_bias.reshape(3, local_width), my_rank * local_width, axis=1
    )
    vector_term = jnp.concatenate(
        [
            from_order(jnp.stack([grad_gain_one, grad_shift_one])),
            bias_rows,
            from_order(jnp.stack([grad_gain_two, grad_shift_two])),
        ]
    )
    vector_grad = sum_vectors(vector_term, 10)
    attention_new, attention_state = adamw_update(
        attention_weights, attention_grad, attention_moments, decay_rate
    )
    feedforward_new, feedforward_state = adamw_update(
        feedforward_weights, feedforward_grad, feedforward_moments, decay_rate
    )
    vector_new, vector_state = adamw_update(norm_vectors, vector_grad, vector_moments, 0.0)
    return (
        from_order(result)[None],
        from_order(grad_stream)[None],
        attention_grad,
        feedforward_grad,
        vector_grad,
        attention_new,
        feedforward_new,
        vector_new,
        attention_state,
        feedforward_state,
        vector_state,
    )


def solution(mesh):
    in_specs = (
        P("fsdp", "seq", None),
        P("fsdp", None),
        P(("seq", "fsdp"), None),
        P(("seq", "fsdp"), None),
        P(None, ("seq", "fsdp")),
        P(None, ("seq", "fsdp"), None),
        P(None, ("seq", "fsdp"), None),
        P(None, None, ("seq", "fsdp")),
        P("fsdp", "seq", None),
    )
    out_specs = (
        P("fsdp", "seq", None),
        P("fsdp", "seq", None),
        P(("seq", "fsdp"), None),
        P(("seq", "fsdp"), None),
        P(None, ("seq", "fsdp")),
        P(("seq", "fsdp"), None),
        P(("seq", "fsdp"), None),
        P(None, ("seq", "fsdp")),
        P(None, ("seq", "fsdp"), None),
        P(None, ("seq", "fsdp"), None),
        P(None, None, ("seq", "fsdp")),
    )

    return jax.shard_map(body, mesh=mesh, in_specs=in_specs, out_specs=out_specs, check_vma=False)
```

```python
import jax
import jax.numpy as jnp
from jax import lax
from jax.experimental import pallas as pl
from jax.experimental.pallas import tpu as pltpu
from jax.sharding import PartitionSpec as P

D = 2048
H = 32
HD = 64
ROT = 16
FF = 5632

norm_epsilon = 1e-05
rope_base = 10000.0
neg_fill = -1e30
learn_rate = 0.01
beta_first = 0.9
beta_second = 0.95
adam_epsilon = 1e-08
decay_rate = 0.1
adam_step = 2.0

MESH_IDS = pl.DeviceIdType.MESH
BOTH = ("seq", "fsdp")
bf16 = jnp.bfloat16
f32 = jnp.float32


def document_positions(segment_ids):
    length = segment_ids.shape[0]
    indices = jnp.arange(length, dtype=jnp.int32)
    changes = jnp.concatenate(
        [jnp.ones((1,), dtype=jnp.bool_), segment_ids[1:] != segment_ids[:-1]]
    )
    starts = lax.cummax(jnp.where(changes, indices, jnp.zeros_like(indices)), axis=0)
    return indices - starts


def rotary_tables(positions, half_rot):
    powers = jnp.arange(half_rot, dtype=jnp.float32) / float(half_rot)
    inverse = rope_base ** (-powers)
    angles = positions.astype(jnp.float32)[:, None] * inverse[None, :]
    return (jnp.cos(angles), jnp.sin(angles))


def rotate(values, cosine, sine, half_rot, direction):
    first = values[..., :half_rot]
    second = values[..., half_rot : 2 * half_rot]
    cosine_wide = cosine[:, None, :]
    sine_wide = sine[:, None, :] * direction
    return jnp.concatenate(
        [
            first * cosine_wide - second * sine_wide,
            second * cosine_wide + first * sine_wide,
            values[..., 2 * half_rot :],
        ],
        axis=-1,
    )


def norm_forward(values, gain, shift):
    centred = values - jnp.mean(values, axis=-1, keepdims=True)
    inverse = lax.rsqrt(jnp.mean(centred * centred, axis=-1, keepdims=True) + norm_epsilon)
    normal_part = centred * inverse
    return (normal_part * gain + shift, normal_part, inverse)


def norm_backward(upstream, normal_part, inverse, gain):
    scaled = upstream * gain
    return inverse * (
        scaled
        - jnp.mean(scaled, axis=-1, keepdims=True)
        - normal_part * jnp.mean(scaled * normal_part, axis=-1, keepdims=True)
    )


def contract_rows(left, right, out=jnp.float32):
    return lax.dot_general(left, right, (((0,), (0,)), ((), ())), preferred_element_type=out)


def contract_cols(left, right, out=jnp.float32):
    return lax.dot_general(left, right, (((1,), (1,)), ((), ())), preferred_element_type=out)


def block_mask(segment_ids, start_row, block_rows):
    total_keys = segment_ids.shape[0]
    row_ids = start_row + jnp.arange(block_rows, dtype=jnp.int32)
    col_ids = jnp.arange(total_keys, dtype=jnp.int32)
    row_segments = lax.dynamic_slice_in_dim(segment_ids, start_row, block_rows)
    return (col_ids[None, :] <= row_ids[:, None]) & (segment_ids[None, :] == row_segments[:, None])


def adamw_terms(weight, grad, first_moment, second_moment, decay):
    first = beta_first * first_moment + (1.0 - beta_first) * grad
    second = beta_second * second_moment + (1.0 - beta_second) * grad * grad
    correct_one = 1.0 - beta_first**adam_step
    correct_two = 1.0 - beta_second**adam_step
    update = first / correct_one / (jnp.sqrt(second / correct_two) + adam_epsilon)
    return weight - learn_rate * (update + decay * weight), first, second


def adamw_update(weight, grad, moments, decay):
    new, first, second = adamw_terms(weight, grad, moments[0], moments[1], decay)
    return new, jnp.stack([first, second])


def adamw_kernel(places, chunk, w_ref, m_ref, *refs):
    *piece_refs, g_ref, new_ref, state_ref = refs
    for ref, moves in zip(piece_refs, places):
        for index, source, target, width in moves:
            values = ref[:, source : source + width] if index is None else ref[index, :, source : source + width]
            g_ref[:, target : target + width] = values.astype(f32)

    @pl.loop(0, g_ref.shape[1] // chunk)
    def _(step):
        cols = pl.ds(pl.multiple_of(step * chunk, chunk), chunk)
        new, first, second = adamw_terms(
            w_ref[:, cols], g_ref[:, cols], m_ref[0, :, cols], m_ref[1, :, cols], decay_rate
        )
        new_ref[:, cols] = new
        state_ref[0, :, cols] = first
        state_ref[1, :, cols] = second


def adamw_pieces(weight, moments, pieces, places, chunk):
    rows, cols = weight.shape
    step = min(16, rows)
    wide = pl.BlockSpec((step, cols), lambda i: (i, 0))
    pair = pl.BlockSpec((2, step, cols), lambda i: (0, i, 0))
    piece_specs = []
    for piece in pieces:
        if piece.ndim == 3:
            piece_specs.append(
                pl.BlockSpec((piece.shape[0], step, piece.shape[2]), lambda i: (0, i, 0))
            )
        else:
            piece_specs.append(pl.BlockSpec((step, piece.shape[1]), lambda i: (i, 0)))
    return pl.pallas_call(
        lambda *refs: adamw_kernel(places, chunk, *refs),
        grid=(rows // step,),
        out_shape=(
            jax.ShapeDtypeStruct((rows, cols), f32),
            jax.ShapeDtypeStruct((rows, cols), f32),
            jax.ShapeDtypeStruct((2, rows, cols), f32),
        ),
        in_specs=[wide, pair, *piece_specs],
        out_specs=(wide, wide, pair),
        compiler_params=pltpu.CompilerParams(vmem_limit_bytes=48 << 20),
        cost_estimate=pl.CostEstimate(
            flops=16 * rows * cols, bytes_accessed=30 * rows * cols, transcendentals=rows * cols
        ),
        name="adamw_pieces",
    )(weight, moments, *pieces)


def plane_places():
    me = lax.axis_index("seq")
    core = me % 2
    first = 2 + 2 * core
    second = 4 - 2 * core
    bit_first = (me // first) % 2
    bit_second = (me // second) % 2
    sibling = me + 1 - 2 * core
    near = me + first * (1 - 2 * bit_first)
    far = me + second * (1 - 2 * bit_second)
    corner = near + second * (1 - 2 * bit_second)
    return me, sibling, near, far, corner


def greet(others):
    barrier = pltpu.get_barrier_semaphore()
    for other in others:
        pl.semaphore_signal(barrier, inc=1, device_id=other, device_id_type=MESH_IDS)
    pl.semaphore_wait(barrier, len(others))


def gather_kernel(x_ref, o_ref, local_sem, send_sem, recv_sem):
    me, sibling, near, far, corner = plane_places()

    def copy(source, slot, index, target):
        return pltpu.make_async_remote_copy(
            src_ref=source,
            dst_ref=o_ref.at[slot],
            send_sem=send_sem.at[index],
            recv_sem=recv_sem.at[index],
            device_id={"seq": target},
            device_id_type=MESH_IDS,
        )

    greet([{"seq": other} for other in (sibling, near, far)])
    own = pltpu.make_async_copy(x_ref, o_ref.at[me], local_sem)
    own.start()
    to_near = copy(x_ref, me, 0, near)
    to_far = copy(x_ref, me, 1, far)
    to_sibling = copy(x_ref, me, 2, sibling)
    to_near.start()
    to_far.start()
    to_sibling.start()
    to_near.wait_recv()
    near_far = copy(o_ref.at[near], near, 3, far)
    near_far.start()
    near_sibling = copy(o_ref.at[near], near, 4, sibling)
    near_sibling.start()
    to_far.wait_recv()
    far_sibling = copy(o_ref.at[far], far, 5, sibling)
    far_sibling.start()
    near_far.wait_recv()
    corner_sibling = copy(o_ref.at[corner], corner, 6, sibling)
    corner_sibling.start()
    for one in (to_sibling, near_sibling, far_sibling, corner_sibling):
        one.wait_recv()
    for one in (to_near, to_far, to_sibling, near_far, near_sibling, far_sibling, corner_sibling):
        one.wait_send()
    own.wait()


def plane_gather(values, collective_id):
    rows, cols = values.shape
    out = pl.pallas_call(
        gather_kernel,
        out_shape=jax.ShapeDtypeStruct((8, rows, cols), values.dtype),
        in_specs=[pl.BlockSpec(memory_space=pltpu.VMEM)],
        out_specs=pl.BlockSpec(memory_space=pl.ANY),
        scratch_shapes=[
            pltpu.SemaphoreType.DMA,
            pltpu.SemaphoreType.DMA((7,)),
            pltpu.SemaphoreType.DMA((7,)),
        ],
        compiler_params=pltpu.CompilerParams(collective_id=collective_id, has_side_effects=True),
        name="plane_gather",
    )(values)
    return out.reshape(8 * rows, cols)


def scatter_kernel(p_ref, o_ref, mine, pair, near_out, near_in, far_out, far_in, local_sem, send_sem, recv_sem):
    me, sibling, near, far, corner = plane_places()
    flip = sibling - me
    order = (corner, near, far, me)
    sibling_order = (corner, far, near, me)

    def copy(source, target_ref, index, target):
        return pltpu.make_async_remote_copy(
            src_ref=source,
            dst_ref=target_ref,
            send_sem=send_sem.at[index],
            recv_sem=recv_sem.at[index],
            device_id={"seq": target},
            device_id_type=MESH_IDS,
        )

    greet([{"seq": other} for other in (sibling, near, far)])
    pairs = []
    locals_ = []
    for index, block in enumerate(order):
        one = copy(p_ref.at[sibling_order[index] + flip], pair.at[index], index, sibling)
        one.start()
        pairs.append(one)
        own = pltpu.make_async_copy(p_ref.at[block], mine.at[index], local_sem.at[index])
        own.start()
        locals_.append(own)
    for index in range(2):
        pairs[index].wait_recv()
        locals_[index].wait()
        near_out[index] = (mine[index].astype(f32) + pair[index].astype(f32)).astype(near_out.dtype)
        step = copy(near_out.at[index], near_in.at[index], 4 + index, near)
        step.start()
        pairs.append(step)
    for index in range(2, 4):
        pairs[index].wait_recv()
        locals_[index].wait()
    pairs[4].wait_recv()
    far_out[...] = (
        mine[2].astype(f32) + pair[2].astype(f32) + near_in[0].astype(f32)
    ).astype(far_out.dtype)
    last = copy(far_out, far_in, 6, far)
    last.start()
    pairs[5].wait_recv()
    o_ref[...] = mine[3].astype(f32) + pair[3].astype(f32) + near_in[1].astype(f32)
    last.wait_recv()
    o_ref[...] += far_in[...].astype(f32)
    for one in pairs:
        one.wait_send()
    last.wait_send()


def plane_scatter(values, collective_id):
    rows, cols = values.shape
    rows = rows // 8
    return pl.pallas_call(
        scatter_kernel,
        out_shape=jax.ShapeDtypeStruct((rows, cols), f32),
        in_specs=[pl.BlockSpec(memory_space=pl.ANY)],
        out_specs=pl.BlockSpec(memory_space=pltpu.VMEM),
        scratch_shapes=[
            pltpu.VMEM((4, rows, cols), values.dtype),
            pltpu.VMEM((4, rows, cols), values.dtype),
            pltpu.VMEM((2, rows, cols), values.dtype),
            pltpu.VMEM((2, rows, cols), values.dtype),
            pltpu.VMEM((rows, cols), values.dtype),
            pltpu.VMEM((rows, cols), values.dtype),
            pltpu.SemaphoreType.DMA((4,)),
            pltpu.SemaphoreType.DMA((7,)),
            pltpu.SemaphoreType.DMA((7,)),
        ],
        compiler_params=pltpu.CompilerParams(
            collective_id=collective_id, has_side_effects=True, vmem_limit_bytes=32 << 20
        ),
        name="plane_scatter",
    )(values.reshape(8, rows, cols))


def peers(axis, size):
    me = lax.axis_index(axis)
    others = tuple((me + k) % size for k in range(1, size))
    return me, others


def vector_gather_kernel(x_ref, o_ref, send_sem, recv_sem):
    seq, seq_others = peers("seq", 8)
    fsdp, fsdp_others = peers("fsdp", 4)
    greet([{"fsdp": other} for other in fsdp_others] + [{"seq": other} for other in seq_others])
    o_ref[seq, fsdp] = x_ref[...]
    copies = []
    for k, other in enumerate(fsdp_others):
        copies.append(
            pltpu.make_async_remote_copy(
                src_ref=x_ref,
                dst_ref=o_ref.at[seq, fsdp],
                send_sem=send_sem.at[k],
                recv_sem=recv_sem.at[k],
                device_id={"fsdp": other},
                device_id_type=MESH_IDS,
            )
        )
        copies[-1].start()
    for one in copies:
        one.wait_recv()
    for k, other in enumerate(seq_others):
        copies.append(
            pltpu.make_async_remote_copy(
                src_ref=o_ref.at[seq],
                dst_ref=o_ref.at[seq],
                send_sem=send_sem.at[3 + k],
                recv_sem=recv_sem.at[3 + k],
                device_id={"seq": other},
                device_id_type=MESH_IDS,
            )
        )
        copies[-1].start()
    for one in copies[3:]:
        one.wait_recv()
    for one in copies:
        one.wait_send()


def vector_sum_kernel(x_ref, o_ref, part, total, last, send_sem, recv_sem):
    seq, seq_others = peers("seq", 8)
    _, fsdp_others = peers("fsdp", 4)
    greet([{"fsdp": other} for other in fsdp_others] + [{"seq": other} for other in seq_others])
    copies = []
    for k, other in enumerate(seq_others):
        copies.append(
            pltpu.make_async_remote_copy(
                src_ref=x_ref.at[other],
                dst_ref=part.at[k],
                send_sem=send_sem.at[k],
                recv_sem=recv_sem.at[k],
                device_id={"seq": other},
                device_id_type=MESH_IDS,
            )
        )
        copies[-1].start()
    for one in copies:
        one.wait_recv()
    total[...] = x_ref[seq] + jnp.sum(part[...], axis=0)
    for k, other in enumerate(fsdp_others):
        copies.append(
            pltpu.make_async_remote_copy(
                src_ref=total,
                dst_ref=last.at[k],
                send_sem=send_sem.at[7 + k],
                recv_sem=recv_sem.at[7 + k],
                device_id={"fsdp": other},
                device_id_type=MESH_IDS,
            )
        )
        copies[-1].start()
    for one in copies[7:]:
        one.wait_recv()
    o_ref[...] = total[...] + jnp.sum(last[...], axis=0)
    for one in copies:
        one.wait_send()


def gather_vectors(values, collective_id):
    rows = values.shape[1]
    if on_grid():
        padded = jnp.pad(values.astype(f32), ((0, 1), (0, 128 - rows)))
        out = pl.pallas_call(
            vector_gather_kernel,
            out_shape=jax.ShapeDtypeStruct((8, 4, 8, 128), f32),
            in_specs=[pl.BlockSpec(memory_space=pltpu.VMEM)],
            out_specs=pl.BlockSpec(memory_space=pltpu.VMEM),
            scratch_shapes=[pltpu.SemaphoreType.DMA((10,)), pltpu.SemaphoreType.DMA((10,))],
            compiler_params=pltpu.CompilerParams(collective_id=collective_id, has_side_effects=True),
            name="vector_gather",
        )(padded)
        return out[:, :, :7, :rows].transpose(2, 0, 1, 3).reshape(7, D)
    return lax.all_gather(values, BOTH, axis=1, tiled=True).astype(f32)


def sum_vectors(values, collective_id):
    if on_grid():
        blocks = jnp.pad(values.reshape(7, 8, D // 8).transpose(1, 0, 2), ((0, 0), (0, 1), (0, 0)))
        out = pl.pallas_call(
            vector_sum_kernel,
            out_shape=jax.ShapeDtypeStruct((8, D // 8), f32),
            in_specs=[pl.BlockSpec(memory_space=pltpu.VMEM)],
            out_specs=pl.BlockSpec(memory_space=pltpu.VMEM),
            scratch_shapes=[
                pltpu.VMEM((7, 8, D // 8), f32),
                pltpu.VMEM((8, D // 8), f32),
                pltpu.VMEM((3, 8, D // 8), f32),
                pltpu.SemaphoreType.DMA((10,)),
                pltpu.SemaphoreType.DMA((10,)),
            ],
            compiler_params=pltpu.CompilerParams(collective_id=collective_id, has_side_effects=True),
            name="vector_sum",
        )(blocks)
        rows = D // 32
        return lax.dynamic_slice_in_dim(out[:7], lax.axis_index("fsdp") * rows, rows, axis=1)
    return lax.psum_scatter(values, BOTH, scatter_dimension=1, tiled=True)


def on_grid():
    return lax.axis_size("seq") == 8 and lax.axis_size("fsdp") == 4


def after(values, *others):
    return lax.optimization_barrier((values, *others))[0]


def gather_tokens(values, collective_id):
    if lax.axis_size("seq") == 8:
        return plane_gather(values, collective_id)
    return lax.all_gather(values, "seq", axis=0, tiled=True)


def scatter_tokens(values, collective_id):
    if lax.axis_size("seq") == 8:
        return plane_scatter(values.astype(bf16), collective_id)
    return lax.psum_scatter(values, "seq", scatter_dimension=0, tiled=True)


def body(
    stream,
    segments,
    attention_weights,
    feedforward_weights,
    norm_vectors,
    attention_moments,
    feedforward_moments,
    vector_moments,
    cotangent,
):
    groups = lax.axis_size("seq")
    shards = lax.axis_size("fsdp")
    my_rank = lax.axis_index("seq")
    tokens = stream.shape[1]
    length = tokens * groups
    local_heads = H // groups
    local_width = local_heads * HD
    unit_width = FF // groups
    owned_rows = D // (groups * shards)
    plane_rows = groups * owned_rows
    half_rot = ROT // 2
    score_scale = float(HD) ** (-0.5)
    block_rows = min(512, length)
    block_starts = jnp.arange(length // block_rows, dtype=jnp.int32) * block_rows

    def to_order(values):
        lead = values.shape[:-1]
        return values.reshape(*lead, groups, shards, owned_rows).swapaxes(-3, -2).reshape(*lead, D)

    def from_order(values):
        lead = values.shape[:-1]
        return values.reshape(*lead, shards, groups, owned_rows).swapaxes(-3, -2).reshape(*lead, D)

    def spread_columns(values, parts, width):
        blocks = values.reshape(owned_rows, parts, groups, width).transpose(2, 0, 1, 3)
        blocks = blocks.reshape(groups, owned_rows, parts * width)
        moved = lax.all_to_all(blocks, "seq", split_axis=0, concat_axis=0, tiled=True)
        return moved.reshape(plane_rows, parts * width)

    vector_full = gather_vectors(norm_vectors.astype(bf16), 9)
    attention_low = attention_weights.astype(bf16)
    feedforward_low = feedforward_weights.astype(bf16)
    out_weights = lax.all_gather(attention_low[:, 3 * D :], "fsdp", axis=0, tiled=True)
    out_weights = to_order(out_weights)
    qkv_block = spread_columns(attention_low[:, : 3 * D], 3, local_width)
    qkv_weights = lax.all_gather(qkv_block, "fsdp", axis=0, tiled=True)
    down_block = spread_columns(feedforward_low[:, 2 * FF :], 1, unit_width)
    down_weights = lax.all_gather(down_block, "fsdp", axis=0, tiled=True)
    in_block = spread_columns(feedforward_low[:, : 2 * FF], 2, unit_width)
    in_weights = lax.all_gather(in_block, "fsdp", axis=0, tiled=True)

    ordered = to_order(vector_full)
    gain_one, shift_one, gain_two, shift_two = [ordered[i] for i in (0, 1, 5, 6)]
    bias = lax.dynamic_slice_in_dim(
        vector_full[2:5], my_rank * local_width, local_width, axis=1
    ).reshape(3 * local_width)
    segment_ids = segments[0]
    cosine, sine = rotary_tables(document_positions(segment_ids), half_rot)

    inputs = to_order(stream[0])
    upstream = to_order(cotangent[0])
    normed_one, normal_one, inverse_one = norm_forward(inputs, gain_one, shift_one)
    normed_all = gather_tokens(normed_one.astype(bf16), 1)
    cotangent_all = gather_tokens(upstream.astype(bf16), 2)
    projected = (
        jnp.dot(normed_all, qkv_weights, preferred_element_type=f32) + bias
    ).reshape(length, 3, local_heads, HD)
    query_all = rotate(projected[:, 0], cosine, sine, half_rot, 1.0).astype(bf16)
    key_all = rotate(projected[:, 1], cosine, sine, half_rot, 1.0).astype(bf16)
    value_all = projected[:, 2].astype(bf16)

    def forward_block(start_row):
        query_block = lax.dynamic_slice_in_dim(query_all, start_row, block_rows)
        scores = (
            jnp.einsum("bhd,lhd->hbl", query_block, key_all, preferred_element_type=jnp.float32)
            * score_scale
        )
        scores = jnp.where(block_mask(segment_ids, start_row, block_rows)[None], scores, neg_fill)
        row_max = jnp.max(scores, axis=-1, keepdims=True)
        weights_raw = jnp.exp(scores - row_max)
        row_sum = jnp.sum(weights_raw, axis=-1, keepdims=True)
        probability = (weights_raw / row_sum).astype(jnp.bfloat16)
        output_block = jnp.einsum(
            "hbl,lhd->bhd", probability, value_all, preferred_element_type=jnp.float32
        ).astype(jnp.bfloat16)
        return (output_block, (row_max + jnp.log(row_sum))[..., 0])

    output_blocks, logsum_blocks = lax.map(forward_block, block_starts)
    output_heads = output_blocks.reshape(length, local_heads, HD)
    attended = output_heads.reshape(length, local_width)
    hidden = inputs + scatter_tokens(jnp.dot(attended, out_weights, preferred_element_type=f32), 3)
    normed_two, normal_two, inverse_two = norm_forward(hidden, gain_two, shift_two)
    normed_two_all = gather_tokens(normed_two.astype(bf16), 4)
    gate_up = jnp.dot(normed_two_all, in_weights, preferred_element_type=f32)
    gate_part = gate_up[:, :unit_width]
    up_part = gate_up[:, unit_width:]
    sigmoid_gate = jax.nn.sigmoid(gate_part)
    activated = (gate_part * sigmoid_gate * up_part).astype(bf16)
    down_term = contract_rows(cotangent_all, activated).astype(bf16)
    grad_act = jnp.dot(after(cotangent_all, down_term), down_weights, preferred_element_type=f32)
    grad_gate = grad_act * up_part * sigmoid_gate * (1.0 + gate_part * (1.0 - sigmoid_gate))
    grad_up = grad_act * gate_part * sigmoid_gate
    grad_gate_up = jnp.concatenate([grad_gate, grad_up], axis=1).astype(bf16)

    def reduce_rows(term):
        return lax.psum_scatter(term, "fsdp", scatter_dimension=0, tiled=True)

    def collect_rows(total):
        blocks = total.reshape(groups, owned_rows, total.shape[1])
        return lax.all_to_all(blocks, "seq", split_axis=0, concat_axis=0, tiled=True)

    def column_moves(parts, width, start):
        return [
            (group, part * width, start + part * groups * width + group * width, width)
            for part in range(parts)
            for group in range(groups)
        ]

    down_sum = reduce_rows(down_term)
    in_term = contract_rows(normed_two_all, after(grad_gate_up, down_term)).astype(bf16)
    in_sum = reduce_rows(in_term)
    grad_normed_two = scatter_tokens(
        contract_cols(after(grad_gate_up, in_term), in_weights), 5
    )

    grad_hidden = upstream + norm_backward(grad_normed_two, normal_two, inverse_two, gain_two)
    grad_gain_two = jnp.sum(grad_normed_two * normal_two, axis=0)
    grad_shift_two = jnp.sum(grad_normed_two, axis=0)
    grad_hidden_all = gather_tokens(grad_hidden.astype(bf16), 6)
    grad_heads = (
        contract_cols(grad_hidden_all, out_weights).astype(bf16).reshape(length, local_heads, HD)
    )

    def backward_block(carry, items):
        grad_key_sum, grad_value_sum = carry
        start_row, logsum_block = items
        query_block = lax.dynamic_slice_in_dim(query_all, start_row, block_rows)
        output_block = lax.dynamic_slice_in_dim(output_heads, start_row, block_rows)
        grad_block = lax.dynamic_slice_in_dim(grad_heads, start_row, block_rows)
        scores = (
            jnp.einsum("bhd,lhd->hbl", query_block, key_all, preferred_element_type=jnp.float32)
            * score_scale
        )
        scores = jnp.where(block_mask(segment_ids, start_row, block_rows)[None], scores, neg_fill)
        probability = jnp.exp(scores - logsum_block[..., None])
        prob_low = probability.astype(jnp.bfloat16)
        grad_value_sum = grad_value_sum + jnp.einsum(
            "hbl,bhd->lhd", prob_low, grad_block, preferred_element_type=jnp.float32
        )
        grad_prob = jnp.einsum(
            "bhd,lhd->hbl", grad_block, value_all, preferred_element_type=jnp.float32
        )
        row_delta = jnp.sum(
            grad_block.astype(jnp.float32) * output_block.astype(jnp.float32), axis=-1
        )
        row_delta = jnp.transpose(row_delta)[..., None]
        grad_scores = (probability * (grad_prob - row_delta) * score_scale).astype(jnp.bfloat16)
        grad_query = jnp.einsum(
            "hbl,lhd->bhd", grad_scores, key_all, preferred_element_type=jnp.float32
        ).astype(jnp.bfloat16)
        grad_key_sum = grad_key_sum + jnp.einsum(
            "hbl,bhd->lhd", grad_scores, query_block, preferred_element_type=jnp.float32
        )
        return ((grad_key_sum, grad_value_sum), grad_query)

    zero_heads = jnp.zeros((length, local_heads, HD), jnp.float32)
    sums, grad_query_blocks = lax.scan(
        backward_block, (zero_heads, zero_heads), (block_starts, logsum_blocks)
    )
    grad_key_sum, grad_value_sum = sums
    grad_query_low = grad_query_blocks.reshape(length, local_heads, HD)
    grad_projected = jnp.concatenate(
        [
            rotate(grad_query_low.astype(f32), cosine, sine, half_rot, -1.0).reshape(
                length, local_width
            ),
            rotate(
                lax.optimization_barrier(grad_key_sum.astype(bf16)).astype(f32),
                cosine,
                sine,
                half_rot,
                -1.0,
            ).reshape(length, local_width),
            lax.optimization_barrier(grad_value_sum.astype(bf16)).astype(f32).reshape(
                length, local_width
            ),
        ],
        axis=1,
    )
    grad_bias = jnp.sum(grad_projected, axis=0)
    grad_projected_low = grad_projected.astype(bf16)
    qkv_term = contract_rows(normed_all, grad_projected_low).astype(bf16)
    qkv_sum = reduce_rows(qkv_term)
    out_term = contract_rows(attended, after(grad_hidden_all, qkv_term)).astype(bf16)
    out_sum = reduce_rows(out_term)
    grad_normed_one = scatter_tokens(
        contract_cols(after(grad_projected_low, out_term), qkv_weights), 8
    )
    grad_stream = grad_hidden + norm_backward(grad_normed_one, normal_one, inverse_one, gain_one)
    grad_gain_one = jnp.sum(grad_normed_one * normal_one, axis=0)
    grad_shift_one = jnp.sum(grad_normed_one, axis=0)

    bias_rows = lax.dynamic_update_slice_in_dim(
        jnp.zeros((3, D), f32), grad_bias.reshape(3, local_width), my_rank * local_width, axis=1
    )
    vector_term = jnp.concatenate(
        [
            from_order(jnp.stack([grad_gain_one, grad_shift_one])),
            bias_rows,
            from_order(jnp.stack([grad_gain_two, grad_shift_two])),
        ]
    )
    vector_grad = sum_vectors(vector_term, 10)
    result = hidden + scatter_tokens(
        contract_cols(after(activated, vector_grad), down_weights), 7
    )
    in_moved = collect_rows(after(in_sum, vector_grad))
    down_moved = collect_rows(down_sum)
    qkv_moved = collect_rows(after(qkv_sum, result, in_moved))
    feedforward_grad, feedforward_new, feedforward_state = adamw_pieces(
        feedforward_weights,
        feedforward_moments,
        [after(in_moved, result), after(down_moved, result)],
        [column_moves(2, unit_width, 0), column_moves(1, unit_width, 2 * FF)],
        1408,
    )
    attention_grad, attention_new, attention_state = adamw_pieces(
        attention_weights,
        attention_moments,
        [after(qkv_moved, feedforward_grad), from_order(after(out_sum, feedforward_grad))],
        [column_moves(3, local_width, 0), [(None, 0, 3 * D, D)]],
        1024,
    )
    vector_new, vector_state = adamw_update(norm_vectors, vector_grad, vector_moments, 0.0)
    return (
        from_order(result)[None],
        from_order(grad_stream)[None],
        attention_grad,
        feedforward_grad,
        vector_grad,
        attention_new,
        feedforward_new,
        vector_new,
        attention_state,
        feedforward_state,
        vector_state,
    )


def solution(mesh):
    in_specs = (
        P("fsdp", "seq", None),
        P("fsdp", None),
        P(("seq", "fsdp"), None),
        P(("seq", "fsdp"), None),
        P(None, ("seq", "fsdp")),
        P(None, ("seq", "fsdp"), None),
        P(None, ("seq", "fsdp"), None),
        P(None, None, ("seq", "fsdp")),
        P("fsdp", "seq", None),
    )
    out_specs = (
        P("fsdp", "seq", None),
        P("fsdp", "seq", None),
        P(("seq", "fsdp"), None),
        P(("seq", "fsdp"), None),
        P(None, ("seq", "fsdp")),
        P(("seq", "fsdp"), None),
        P(("seq", "fsdp"), None),
        P(None, ("seq", "fsdp")),
        P(None, ("seq", "fsdp"), None),
        P(None, ("seq", "fsdp"), None),
        P(None, None, ("seq", "fsdp")),
    )

    return jax.shard_map(body, mesh=mesh, in_specs=in_specs, out_specs=out_specs, check_vma=False)
```
